512 devices in a mesh: pb: 8 (over y_lo, x), ka: 16 (over z, core), ha: 4 (over y_hi).
Axes of the slice: x: 4, y: 8 (y_hi: 4, y_lo: 2; y = y_hi * 2 + y_lo), z: 8, core: 2. Of those that a mesh axis runs over, the one named last changes fastest.
Arguments:
- queries: bfloat16 [3072, 64, 128], P('pb', 'ha'), may hold values from -6 to 6
- key_codes: bfloat16 [3072, 8, 128], P('ka', 'ha'), may hold values from -4 to 4
- key_scale_powers: int32 [48, 8], P('ka', 'ha'), may hold values from -1 to 1
- values: bfloat16 [3072, 8, 128], P('ka', 'ha'), may hold values from -6 to 6
- grad_out: bfloat16 [3072, 64, 128], P('pb', 'ha'), may hold values from -1.5 to 1.5
- grad_dot: float32 [3072, 64], P('pb', 'ha'), may hold values from -6 to 6
- log_totals: float32 [3072, 64], P('pb', 'ha')
Outputs:
- grad_queries: bfloat16 [3072, 64, 128], P(('pb', 'ka'), 'ha')
- grad_keys: bfloat16 [3072, 8, 128], P('ka', 'ha')
- grad_values: bfloat16 [3072, 8, 128], P('ka', 'ha')
The draws below stay inside these ranges and needn't reach their ends.
All inputs are finite; a program needn't handle non-finite values.
Results may differ from the reference program's by a relative error of at most 0.012.
Values may be sent and summed in bfloat16 or wider, within the bound.
A program may use at most 64 MiB of HBM per device.

```python
import jax
import jax.numpy as jnp
from jax import lax

KEY_VALUE_HEADS = 8
HEAD_SIZE = 128
KEYS_PER_SCALE = 64
QUERY_HEADS = 64
WINDOW_TOKENS = 3072


def draw_key_codes(key, part):
    first_part, second_part = jax.random.split(jax.random.fold_in(key, 11))
    start_offsets = jax.random.uniform(first_part, (1, KEY_VALUE_HEADS, HEAD_SIZE), jnp.float32, -0.4, 0.4)
    fraction = jnp.arange(WINDOW_TOKENS, dtype=jnp.float32)[:, None, None] / (WINDOW_TOKENS - 1)
    ramp = 1.0 + 2.0 * fraction
    random_jitter = 0.6 * jax.random.normal(second_part, (WINDOW_TOKENS, KEY_VALUE_HEADS, HEAD_SIZE), jnp.float32)
    return jnp.clip(start_offsets * ramp + random_jitter, -4.0, 4.0).astype(jnp.bfloat16)


def draw_log_totals(key, part):
    inner = jax.random.fold_in(key, 23)
    level = jnp.log(1.0 + WINDOW_TOKENS * jnp.ones((WINDOW_TOKENS, 1), jnp.float32))
    extra = jax.random.uniform(inner, (WINDOW_TOKENS, QUERY_HEADS), jnp.float32, 0.5, 1.5)
    return level + extra


def touch_ends(entries, rng, low, top_value):
    spot = [jax.random.randint(jax.random.fold_in(rng, axis), (), 0, length) for axis, length in enumerate(entries.shape)]
    longest = entries.shape.index(max(entries.shape))
    neighbour = spot[:longest] + [(spot[longest] + 1) % entries.shape[longest]] + spot[longest + 1:]
    return entries.at[tuple(spot)].set(low).at[tuple(neighbour)].set(top_value)


def block_levels(own_key, shape, shards, smallest, high):
    factor_of, own = 1.0, jax.random.fold_in(own_key, 6)
    for axis_at, parts in shards:
        steps = jnp.exp(jax.random.uniform(jax.random.fold_in(own, axis_at), (parts,), jnp.float32, smallest / len(shards), high / len(shards)))
        factor_of = factor_of * jnp.repeat(steps, shape[axis_at] // parts).reshape([-1 if axis == axis_at else 1 for axis in range(len(shape))])
    return factor_of


def gaussian(key, extent, scale, most, pieces=(), kind=jnp.bfloat16):
    entries = scale * jax.random.normal(key, extent, jnp.float32)
    if pieces:
        entries = entries * block_levels(key, extent, pieces, -0.22, 0.18)
    return jnp.clip(entries, -most, most).astype(kind)


def setup_inputs(seed: int = 0) -> dict:
    arg_keys = jax.random.split(jax.random.key(seed), 8)
    queries = gaussian(arg_keys[0], (WINDOW_TOKENS, QUERY_HEADS, HEAD_SIZE), 1.0, 6.0, ((0, 8), (1, 4)))
    key_codes = draw_key_codes(jax.random.fold_in(arg_keys[7], 71), 0)
    key_scale_powers = touch_ends(jax.random.randint(arg_keys[2], (WINDOW_TOKENS // KEYS_PER_SCALE, KEY_VALUE_HEADS), -1, 2), jax.random.fold_in(arg_keys[2], 1), -1, 1).astype(jnp.int32)
    values = gaussian(arg_keys[3], (WINDOW_TOKENS, KEY_VALUE_HEADS, HEAD_SIZE), 1.0, 6.0, ((0, 16), (1, 4)))
    grad_out = gaussian(arg_keys[4], (WINDOW_TOKENS, QUERY_HEADS, HEAD_SIZE), 0.25, 1.5, ((0, 8), (1, 4)))
    grad_dot = gaussian(arg_keys[5], (WINDOW_TOKENS, QUERY_HEADS), 1.0, 6.0, ((0, 8), (1, 4)), jnp.float32)
    log_totals = draw_log_totals(jax.random.fold_in(arg_keys[7], 71), 0)
    return dict(queries=queries, key_codes=key_codes, key_scale_powers=key_scale_powers, values=values, grad_out=grad_out, grad_dot=grad_dot, log_totals=log_totals)


def grads_one(item):
    query_block, grad_block, dot_block, total_block, key_block, value_block = item
    inverse_root = HEAD_SIZE ** -0.5
    positions = jnp.arange(WINDOW_TOKENS, dtype=jnp.int32)
    visible = positions[None, :] <= positions[:, None]
    query_wide = query_block.astype(jnp.float32)
    grad_wide = grad_block.astype(jnp.float32)
    key_wide = key_block.astype(jnp.float32)
    value_wide = value_block.astype(jnp.float32)
    scores = jnp.einsum("igd,jd->gij", query_wide, key_wide) * inverse_root
    weights = jnp.where(visible[None], jnp.exp(scores - total_block.T[:, :, None]), 0.0)
    weights_low = weights.astype(jnp.bfloat16).astype(jnp.float32)
    grad_values = jnp.einsum("gij,igd->jd", weights_low, grad_wide)
    grad_weights = jnp.einsum("igd,jd->gij", grad_wide, value_wide)
    grad_scores = (weights * (grad_weights - dot_block.T[:, :, None])).astype(jnp.bfloat16).astype(jnp.float32)
    grad_query = jnp.einsum("gij,jd->igd", grad_scores, key_wide) * inverse_root
    grad_keys = jnp.einsum("gij,igd->jd", grad_scores, query_wide) * inverse_root
    return grad_query.astype(jnp.bfloat16), grad_keys.astype(jnp.bfloat16), grad_values.astype(jnp.bfloat16)


def reference(queries, key_codes, key_scale_powers, values, grad_out, grad_dot, log_totals):
    queries_per_group = QUERY_HEADS // KEY_VALUE_HEADS
    factor = jnp.exp2(key_scale_powers.astype(jnp.float32))
    dequantized = key_codes.astype(jnp.float32) * jnp.repeat(factor, KEYS_PER_SCALE, axis=0)[:, :, None]
    key_means = jnp.sum(dequantized, axis=0) / WINDOW_TOKENS
    smoothed = (dequantized - key_means).astype(jnp.bfloat16)

    def by_group(input_matrix):
        return jnp.swapaxes(input_matrix.reshape((WINDOW_TOKENS, KEY_VALUE_HEADS, queries_per_group) + input_matrix.shape[2:]), 0, 1)

    items = (by_group(queries), by_group(grad_out), by_group(grad_dot), by_group(log_totals),
             jnp.swapaxes(smoothed, 0, 1), jnp.swapaxes(values, 0, 1))
    grad_query, grad_keys, grad_values = lax.map(grads_one, items)
    grad_query = jnp.swapaxes(grad_query, 0, 1).reshape(WINDOW_TOKENS, QUERY_HEADS, HEAD_SIZE)
    return grad_query, jnp.swapaxes(grad_keys, 0, 1), jnp.swapaxes(grad_values, 0, 1)
```

```python
import functools

import jax
import jax.numpy as jnp
from jax import lax
from jax.experimental import pallas as pl
from jax.experimental.pallas import tpu as pltpu
from jax.sharding import PartitionSpec as P

F32 = jnp.float32
BF16 = jnp.bfloat16
MESH = pl.DeviceIdType.MESH
NT = (((1,), (1,)), ((), ()))
NN = (((1,), (0,)), ((), ()))

PB = 8
NZ = 8
KA = 16
TOK = 384
GROUP = 8
D = 128
KEYS = 192
CKEYS = 384
SHARE = 48
ROWS = SHARE * GROUP
HALF = ROWS // 2
PIECE = CKEYS // PB
KEYS_PER_SCALE = 64
LOG2E = 1.4426950408889634


def dot(a, b, dims):
    return lax.dot_general(a, b, dims, preferred_element_type=F32)


def split3(x):
    hi = x.astype(BF16).astype(F32)
    rest = x - hi
    mid = rest.astype(BF16).astype(F32)
    return hi, mid, rest - mid


def kernel(
    q_hbm, go_hbm, tot_ref, dots_ref, codes_ref, vals_ref, pows_ref,
    dq_ref, dkv_ref,
    qbuf, gobuf, q2, go2, mbuf, deq, kv_full, sums, means, kt, s_all, dp_all,
    p_scr, ds_scr, dqbuf, acc, tx, rx, fin, sib, kvtx, kvrx, red, ag,
    in_sem, kvx_s, kvx_r, mean_s, mean_r, tx_s, rx_r, fin_r, sib_r,
    pb_s, pb_r, ag_s, ag_r,
):
    b = lax.axis_index("pb")
    ka = lax.axis_index("ka")
    z = ka // 2
    c = ka % 2
    other = 1 - c
    sibling = 2 * z + other
    inv = D ** -0.5

    barrier = pltpu.get_barrier_semaphore()
    for k in range(1, KA):
        pl.semaphore_signal(barrier, inc=1, device_id={"ka": (ka + k) % KA}, device_id_type=MESH)
    for k in range(1, PB):
        for core in range(2):
            pl.semaphore_signal(
                barrier, inc=1, device_id={"pb": (b + k) % PB, "ka": 2 * z + core}, device_id_type=MESH
            )

    q_copy = pltpu.make_async_copy(q_hbm.at[:, c], qbuf, in_sem.at[0])
    go_copy = pltpu.make_async_copy(go_hbm.at[:, c], gobuf, in_sem.at[1])
    q_copy.start()
    go_copy.start()

    both = jnp.concatenate([codes_ref[...], vals_ref[...]], axis=1)
    for h in range(2):
        row = lax.broadcasted_iota(jnp.int32, (KEYS, 2 * KEYS), 0)
        col = lax.broadcasted_iota(jnp.int32, (KEYS, 2 * KEYS), 1)
        pick = jnp.where(col == 2 * row + h, 1.0, 0.0).astype(BF16)
        picked = dot(pick, both, NN)
        total = jnp.zeros((1, D), F32)
        for blk in range(KEYS // KEYS_PER_SCALE):
            at = slice(blk * KEYS_PER_SCALE, (blk + 1) * KEYS_PER_SCALE)
            power = jnp.full((KEYS_PER_SCALE, D), pows_ref[blk, h], jnp.int32).astype(F32)
            scaled = picked[at, :D] * jnp.exp2(power)
            total = total + jnp.sum(scaled, axis=0, keepdims=True)
            deq[h, 0, at, :] = scaled.astype(BF16)
        deq[h, 1, :, :] = picked[:, D:].astype(BF16)
        sums[h] = jnp.broadcast_to(total, (8, D))

    own_rows = pl.ds(pl.multiple_of(KEYS * c, KEYS), KEYS)
    kv_full[:, own_rows, :] = deq[c]

    heads = pl.ds(pl.multiple_of(GROUP * c, GROUP), GROUP)
    pieces = split3(tot_ref[heads, :] * (D ** 0.5)) + split3(dots_ref[heads, :])
    stacked = jnp.concatenate(list(pieces) + [jnp.zeros((D - 6 * GROUP, TOK), F32)], axis=0)
    by_token = stacked.T
    lane = lax.broadcasted_iota(jnp.int32, (GROUP, D), 1)
    sub = lax.broadcasted_iota(jnp.int32, (GROUP, D), 0)
    own_lane = jnp.where((lane & (GROUP - 1)) == sub, 1.0, 0.0)
    for s in range(NZ):
        at = by_token[s * SHARE:(s + 1) * SHARE]
        spread = at[:, None, :] * own_lane[None]
        mbuf[s * ROWS:(s + 1) * ROWS, :] = spread.reshape(ROWS, D).astype(BF16)

    q_copy.wait()
    go_copy.wait()

    def flatten(s, carry):
        toks = pl.ds(s * SHARE, SHARE)
        rows = pl.ds(pl.multiple_of(s * ROWS, ROWS), ROWS)
        q2[rows, :] = qbuf[toks].astype(F32).reshape(ROWS, D).astype(BF16)
        go2[rows, :] = gobuf[toks].astype(F32).reshape(ROWS, D).astype(BF16)
        return carry

    lax.fori_loop(0, NZ, flatten, 0)

    pl.semaphore_wait(barrier, KA - 1 + 2 * (PB - 1))

    def mean_copy(k):
        peer = (ka + k) % KA
        return pltpu.make_async_remote_copy(
            src_ref=sums.at[peer % 2], dst_ref=means.at[ka], send_sem=mean_s.at[k],
            recv_sem=mean_r.at[ka], device_id={"ka": peer}, device_id_type=MESH,
        )

    def mean_arrival(k):
        peer = (ka + k) % KA
        return pltpu.make_async_remote_copy(
            src_ref=sums.at[c], dst_ref=means.at[peer], send_sem=mean_s.at[k],
            recv_sem=mean_r.at[peer], device_id={"ka": peer}, device_id_type=MESH,
        )

    swap = pltpu.make_async_remote_copy(
        src_ref=deq.at[other], dst_ref=kv_full.at[:, own_rows], send_sem=kvx_s, recv_sem=kvx_r,
        device_id={"ka": sibling}, device_id_type=MESH,
    )
    their_rows = pl.ds(pl.multiple_of(KEYS * other, KEYS), KEYS)
    swapped = pltpu.make_async_remote_copy(
        src_ref=deq.at[other], dst_ref=kv_full.at[:, their_rows], send_sem=kvx_s, recv_sem=kvx_r,
        device_id={"ka": sibling}, device_id_type=MESH,
    )
    for k in range(1, KA):
        mean_copy(k).start()
    swap.start()
    swapped.wait_recv()

    lanes = lax.broadcasted_iota(jnp.int32, (CKEYS, D), 1)
    k_ones = jnp.where(lanes < 3 * GROUP, -1.0, 0.0).astype(BF16)
    v_ones = jnp.where((lanes >= 3 * GROUP) & (lanes < 6 * GROUP), -1.0, 0.0).astype(BF16)

    def first(s, carry):
        rows = pl.ds(pl.multiple_of(s * ROWS, ROWS), ROWS)
        extra = mbuf[rows, :]
        k_in = jnp.concatenate([kv_full[0], k_ones], axis=1)
        v_in = jnp.concatenate([kv_full[1], v_ones], axis=1)
        s_all[s] = dot(k_in, jnp.concatenate([q2[rows, :], extra], axis=1), NT)
        dp_all[s] = dot(v_in, jnp.concatenate([go2[rows, :], extra], axis=1), NT)
        return carry

    lax.fori_loop(0, NZ, first, 0)

    for k in range(1, KA):
        mean_arrival(k).wait_recv()
    means[ka] = sums[c]
    mean = jnp.sum(means[...], axis=0) / (KA * KEYS)
    smoothed = kv_full[0].astype(F32) - mean[0:1]
    kt[...] = smoothed.T.astype(BF16)
    m_hi, m_mid, m_lo = split3(mean)
    srow = lax.broadcasted_iota(jnp.int32, (8, D), 0)
    mean_rows = jnp.where(srow == 0, m_hi, jnp.where(srow == 1, m_mid, jnp.where(srow == 2, m_lo, 0.0)))
    mean_rows = jnp.concatenate([mean_rows, jnp.zeros((8, D), F32)], axis=0).astype(BF16)
    acc[...] = jnp.zeros_like(acc)

    def offset(t):
        return jnp.where(t % 2 == 1, (t - 1) // 2 - 3, NZ // 2 - t // 2)

    left = (z + NZ - 1) % NZ
    right = (z + 1) % NZ

    def hop(t, half):
        leftward = half == 0 if t == 0 else t % 2 == 1
        to = left if leftward else right
        if t < 5:
            at = (1 if half == 0 else 2) if t == 0 else t + 2
            return pltpu.make_async_remote_copy(
                src_ref=tx.at[t, half], dst_ref=rx.at[at, half], send_sem=tx_s.at[t, half],
                recv_sem=rx_r.at[at, half], device_id={"ka": 2 * to + c}, device_id_type=MESH,
            )
        side = 0 if leftward else 1
        return pltpu.make_async_remote_copy(
            src_ref=tx.at[t, half], dst_ref=fin.at[side, c], send_sem=tx_s.at[t, half],
            recv_sem=fin_r.at[side, c], device_id={"ka": 2 * to + half}, device_id_type=MESH,
        )

    def arrival(t, half):
        return pltpu.make_async_remote_copy(
            src_ref=tx.at[t, half], dst_ref=rx.at[t, half], send_sem=tx_s.at[t, half],
            recv_sem=rx_r.at[t, half], device_id={"ka": sibling}, device_id_type=MESH,
        )

    def part(t, half):
        return dqbuf[t, half * HALF:(half + 1) * HALF, :]

    def begin(t, half):
        tx[t, half] = part(t, half).astype(BF16)
        hop(t, half).start()

    def forward(t, half):
        arrival(t, half).wait_recv()
        tx[t, half] = (part(t, half) + rx[t, half].astype(F32)).astype(BF16)
        hop(t, half).start()

    def second(t, carry):
        s = (z + offset(t) + NZ) % NZ
        rows = pl.ds(pl.multiple_of(s * ROWS, ROWS), ROWS)
        q_in = q2[rows, :]
        go_in = go2[rows, :]
        shift = jnp.sum(dot(mean_rows, q_in, NT)[0:8], axis=0, keepdims=True)
        limit = TOK * b + SHARE * s - CKEYS * z
        token = lax.shift_right_logical(lax.broadcasted_iota(jnp.int32, (16, ROWS), 1), 3)
        gap = lax.broadcasted_iota(jnp.int32, (16, ROWS), 0) - token
        for k0 in range(0, CKEYS, 16):
            scores = (s_all[s, k0:k0 + 16, :] - shift) * (inv * LOG2E)
            w = jnp.where(gap + k0 <= limit, jnp.exp2(scores), 0.0)
            p_scr[k0:k0 + 16, :] = w.astype(BF16)
            ds_scr[k0:k0 + 16, :] = (w * dp_all[s, k0:k0 + 16, :]).astype(BF16)
        p_in = p_scr[...]
        ds_in = ds_scr[...]
        dqbuf[t] = (dot(kt[...], ds_in, NN) * inv).T
        acc[0] += dot(ds_in, q_in, NN)
        acc[1] += dot(p_in, go_in, NN)

        @pl.when(t == 0)
        def _():
            begin(0, 0)
            begin(0, 1)

        @pl.when(t == 1)
        def _():
            begin(1, 1)

        @pl.when(t == 2)
        def _():
            begin(2, 0)

        @pl.when(t == 4)
        def _():
            forward(1, 0)
            forward(2, 1)

        return carry

    lax.fori_loop(0, NZ, second, 0)

    kvtx[0] = (acc[0] * inv).astype(BF16)
    kvtx[1] = acc[1].astype(BF16)

    def piece_copy(k):
        peer = (b + k) % PB
        return pltpu.make_async_remote_copy(
            src_ref=kvtx.at[:, pl.ds(pl.multiple_of(peer * PIECE, PIECE), PIECE)], dst_ref=kvrx.at[b],
            send_sem=pb_s.at[k], recv_sem=pb_r.at[b], device_id={"pb": peer}, device_id_type=MESH,
        )

    def piece_arrival(k):
        peer = (b + k) % PB
        return pltpu.make_async_remote_copy(
            src_ref=kvtx.at[:, pl.ds(pl.multiple_of(peer * PIECE, PIECE), PIECE)], dst_ref=kvrx.at[peer],
            send_sem=pb_s.at[k], recv_sem=pb_r.at[peer], device_id={"pb": peer}, device_id_type=MESH,
        )

    for k in range(1, PB):
        piece_copy(k).start()

    tx[7, 0] = part(7, 0).astype(BF16)
    tx[7, 1] = part(7, 1).astype(BF16)
    to_sib = pltpu.make_async_remote_copy(
        src_ref=tx.at[7, other], dst_ref=sib, send_sem=tx_s.at[7, 0], recv_sem=sib_r,
        device_id={"ka": sibling}, device_id_type=MESH,
    )
    to_sib.start()

    for t in (3, 4, 5, 6):
        for half in range(2):
            forward(t, half)

    for k in range(1, PB):
        piece_arrival(k).wait_recv()
    kvrx[b] = kvtx[:, pl.ds(pl.multiple_of(b * PIECE, PIECE), PIECE), :]
    gathered = kvrx[0].astype(F32)
    for k in range(1, PB):
        gathered = gathered + kvrx[k].astype(F32)
    red[...] = gathered.astype(BF16)

    owner = b // (PB // 2)
    slot = b % (PB // 2)
    goal = ag.at[:, c, pl.ds(pl.multiple_of(slot * PIECE, PIECE), PIECE)]

    def spread_copy(k):
        return pltpu.make_async_remote_copy(
            src_ref=red, dst_ref=goal, send_sem=ag_s.at[k], recv_sem=ag_r.at[c, slot],
            device_id={"pb": (b + k) % PB, "ka": 2 * z + owner}, device_id_type=MESH,
        )

    def spread_arrival(h, sl):
        return pltpu.make_async_remote_copy(
            src_ref=red, dst_ref=ag.at[:, h, pl.ds(sl * PIECE, PIECE)], send_sem=ag_s.at[0],
            recv_sem=ag_r.at[h, sl], device_id={"ka": sibling}, device_id_type=MESH,
        )

    for k in range(1, PB):
        spread_copy(k).start()

    @pl.when(owner == c)
    def _():
        ag[:, c, pl.ds(pl.multiple_of(slot * PIECE, PIECE), PIECE), :] = red[...]

    @pl.when(owner != c)
    def _():
        spread_copy(0).start()

    for side in range(2):
        for h in range(2):
            pltpu.make_async_remote_copy(
                src_ref=tx.at[5, 0], dst_ref=fin.at[side, h], send_sem=tx_s.at[5, 0],
                recv_sem=fin_r.at[side, h], device_id={"ka": sibling}, device_id_type=MESH,
            ).wait_recv()
    to_sib.wait_recv()
    mine = dqbuf[7, pl.ds(pl.multiple_of(c * HALF, HALF), HALF), :]
    for h, local in ((c, mine), (other, sib[...].astype(F32))):
        whole = local + fin[0, h].astype(F32) + fin[1, h].astype(F32)
        dq_ref[:, h] = whole.reshape(HALF // GROUP, GROUP, D).astype(BF16)

    for h in range(2):
        for sl in range(PB // 2):
            @pl.when(jnp.logical_not((owner == c) & (slot == sl) & (c == h)))
            def _():
                spread_arrival(h, sl).wait_recv()
    dkv_ref[...] = ag[...]

    for k in range(1, KA):
        mean_copy(k).wait_send()
    swap.wait_send()
    for t in range(7):
        for half in range(2):
            hop(t, half).wait_send()
    to_sib.wait_send()
    for k in range(1, PB):
        piece_copy(k).wait_send()
        spread_copy(k).wait_send()

    @pl.when(owner != c)
    def _():
        spread_copy(0).wait_send()


def per_device(queries, key_codes, key_scale_powers, values, grad_out, grad_dot, log_totals):
    vmem = pl.BlockSpec(memory_space=pltpu.VMEM)
    anyw = pl.BlockSpec(memory_space=pl.ANY)
    dma = pltpu.SemaphoreType.DMA
    dq, dkv = pl.pallas_call(
        kernel,
        out_shape=(
            jax.ShapeDtypeStruct((TOK // KA, 2, GROUP, D), BF16),
            jax.ShapeDtypeStruct((2, 2, KEYS, D), BF16),
        ),
        in_specs=[anyw, anyw, vmem, vmem, vmem, vmem, pl.BlockSpec(memory_space=pltpu.SMEM)],
        out_specs=(vmem, vmem),
        scratch_shapes=[
            pltpu.VMEM((TOK, GROUP, D), BF16),
            pltpu.VMEM((TOK, GROUP, D), BF16),
            pltpu.VMEM((TOK * GROUP, D), BF16),
            pltpu.VMEM((TOK * GROUP, D), BF16),
            pltpu.VMEM((TOK * GROUP, D), BF16),
            pltpu.VMEM((2, 2, KEYS, D), BF16),
            pltpu.VMEM((2, CKEYS, D), BF16),
            pltpu.VMEM((2, 8, D), F32),
            pltpu.VMEM((KA, 8, D), F32),
            pltpu.VMEM((D, CKEYS), BF16),
            pltpu.VMEM((NZ, CKEYS, ROWS), F32),
            pltpu.VMEM((NZ, CKEYS, ROWS), F32),
            pltpu.VMEM((CKEYS, ROWS), BF16),
            pltpu.VMEM((CKEYS, ROWS), BF16),
            pltpu.VMEM((NZ, ROWS, D), F32),
            pltpu.VMEM((2, CKEYS, D), F32),
            pltpu.VMEM((NZ, 2, HALF, D), BF16),
            pltpu.VMEM((7, 2, HALF, D), BF16),
            pltpu.VMEM((2, 2, HALF, D), BF16),
            pltpu.VMEM((HALF, D), BF16),
            pltpu.VMEM((2, CKEYS, D), BF16),
            pltpu.VMEM((PB, 2, PIECE, D), BF16),
            pltpu.VMEM((2, PIECE, D), BF16),
            pltpu.VMEM((2, 2, KEYS, D), BF16),
            dma((2,)),
            dma,
            dma,
            dma((KA,)),
            dma((KA,)),
            dma((NZ, 2)),
            dma((7, 2)),
            dma((2, 2)),
            dma,
            dma((PB,)),
            dma((PB,)),
            dma((PB,)),
            dma((2, PB // 2)),
        ],
        compiler_params=pltpu.CompilerParams(collective_id=0, has_side_effects=True),
    )(
        queries.reshape(TOK, 2, GROUP, D),
        grad_out.reshape(TOK, 2, GROUP, D),
        log_totals.T,
        grad_dot.T,
        key_codes.reshape(2 * KEYS, D),
        values.reshape(2 * KEYS, D),
        key_scale_powers,
    )
    return (
        dq.reshape(TOK // KA, 2 * GROUP, D),
        jnp.swapaxes(dkv[0], 0, 1),
        jnp.swapaxes(dkv[1], 0, 1),
    )


def solution(mesh):
    in_specs = (
        P("pb", "ha", None),
        P("ka", "ha", None),
        P("ka", "ha"),
        P("ka", "ha", None),
        P("pb", "ha", None),
        P("pb", "ha"),
        P("pb", "ha"),
    )
    out_specs = (P(("pb", "ka"), "ha", None), P("ka", "ha", None), P("ka", "ha", None))
    return jax.shard_map(
        per_device, mesh=mesh, in_specs=in_specs, out_specs=out_specs, check_vma=False
    )
```

```python
import functools

import jax
import jax.numpy as jnp
from jax import lax
from jax.experimental import pallas as pl
from jax.experimental.pallas import tpu as pltpu
from jax.sharding import PartitionSpec as P

F32 = jnp.float32
BF16 = jnp.bfloat16
MESH = pl.DeviceIdType.MESH
NT = (((1,), (1,)), ((), ()))
NN = (((1,), (0,)), ((), ()))

PB = 8
NZ = 8
KA = 16
TOK = 384
GROUP = 8
D = 128
KEYS = 192
CKEYS = 384
SHARE = 48
ROWS = SHARE * GROUP
HALF = ROWS // 2
PIECE = CKEYS // PB
KEYS_PER_SCALE = 64
LOG2E = 1.4426950408889634
HIDDEN = -1e30
FAR_FIRST = sorted(range(1, KA), key=lambda k: (abs(k - KA // 2), k))


def dot(a, b, dims):
    return lax.dot_general(a, b, dims, preferred_element_type=F32)


def split3(x):
    hi = x.astype(BF16).astype(F32)
    rest = x - hi
    mid = rest.astype(BF16).astype(F32)
    return hi, mid, rest - mid


def kernel(
    q_hbm, go_hbm, tot_hbm, dots_hbm, codes_hbm, vals_hbm, pows_hbm,
    dq_ref, dkv_ref,
    tot_ref, dots_ref, codes_ref, vals_ref, pows_ref, merge,
    qbuf, gobuf, q2, go2, mbuf, deq, kv_full, sums, means, kt, s_all, dp_all,
    stab, totf, gain, dqt, p_scr, ds_scr, dqbuf, acc, tx, rx, fin, sib, kvtx, kvrx, red, ag,
    in_sem, kvx_s, kvx_r, mean_s, mean_r, tx_s, rx_r, fin_r, sib_r,
    pb_s, pb_r, ag_s, ag_r,
):
    b = lax.axis_index("pb")
    ka = lax.axis_index("ka")
    z = ka // 2
    c = ka % 2
    other = 1 - c
    sibling = 2 * z + other
    inv = D ** -0.5

    barrier = pltpu.get_barrier_semaphore()
    for k in FAR_FIRST:
        pl.semaphore_signal(barrier, inc=1, device_id={"ka": (ka + k) % KA}, device_id_type=MESH)
    for k in range(1, PB):
        for core in range(2):
            pl.semaphore_signal(
                barrier, inc=1, device_id={"pb": (b + k) % PB, "ka": 2 * z + core}, device_id_type=MESH
            )

    q_copy = pltpu.make_async_copy(q_hbm.at[:, c], qbuf, in_sem.at[0])
    go_copy = pltpu.make_async_copy(go_hbm.at[:, c], gobuf, in_sem.at[1])
    heads = pl.ds(pl.multiple_of(GROUP * c, GROUP), GROUP)
    loads = [
        pltpu.make_async_copy(codes_hbm, codes_ref, in_sem.at[2]),
        pltpu.make_async_copy(vals_hbm, vals_ref, in_sem.at[3]),
        pltpu.make_async_copy(pows_hbm, pows_ref, in_sem.at[4]),
        pltpu.make_async_copy(tot_hbm.at[heads], tot_ref, in_sem.at[5]),
        pltpu.make_async_copy(dots_hbm.at[heads], dots_ref, in_sem.at[6]),
    ]
    for load in loads:
        load.start()
    q_copy.start()
    go_copy.start()
    for load in loads:
        load.wait()

    both = jnp.concatenate([codes_ref[...], vals_ref[...]], axis=1)
    for h in range(2):
        row = lax.broadcasted_iota(jnp.int32, (KEYS, 2 * KEYS), 0)
        col = lax.broadcasted_iota(jnp.int32, (KEYS, 2 * KEYS), 1)
        pick = jnp.where(col == 2 * row + h, 1.0, 0.0).astype(BF16)
        picked = dot(pick, both, NN)
        total = jnp.zeros((1, D), F32)
        for blk in range(KEYS // KEYS_PER_SCALE):
            at = slice(blk * KEYS_PER_SCALE, (blk + 1) * KEYS_PER_SCALE)
            power = jnp.full((KEYS_PER_SCALE, D), pows_ref[h, blk], jnp.int32).astype(F32)
            scaled = picked[at, :D] * jnp.exp2(power)
            total = total + jnp.sum(scaled, axis=0, keepdims=True)
            deq[h, 0, at, :] = scaled.astype(BF16)
        deq[h, 1, :, :] = picked[:, D:].astype(BF16)
        sums[h] = total

    own_rows = pl.ds(pl.multiple_of(KEYS * c, KEYS), KEYS)
    kv_full[:, own_rows, :] = deq[c]

    pieces = split3(tot_ref[...] * (D ** 0.5)) + split3(dots_ref[...])
    stacked = jnp.concatenate(list(pieces) + [jnp.zeros((D - 6 * GROUP, TOK), F32)], axis=0)
    by_token = stacked.T
    lane = lax.broadcasted_iota(jnp.int32, (GROUP, D), 1)
    sub = lax.broadcasted_iota(jnp.int32, (GROUP, D), 0)
    own_lane = jnp.where((lane & (GROUP - 1)) == sub, 1.0, 0.0)
    for s in range(NZ):
        at = by_token[s * SHARE:(s + 1) * SHARE]
        spread = at[:, None, :] * own_lane[None]
        mbuf[s * ROWS:(s + 1) * ROWS, :] = spread.reshape(ROWS, D).astype(BF16)

    q_copy.wait()
    go_copy.wait()

    def flatten(s, carry):
        toks = pl.ds(s * SHARE, SHARE)
        rows = pl.ds(pl.multiple_of(s * ROWS, ROWS), ROWS)
        q2[rows, :] = qbuf[toks].astype(F32).reshape(ROWS, D).astype(BF16)
        go2[rows, :] = gobuf[toks].astype(F32).reshape(ROWS, D).astype(BF16)
        return carry

    lax.fori_loop(0, NZ, flatten, 0)

    pl.semaphore_wait(barrier, KA - 1 + 2 * (PB - 1))

    def mean_copy(k):
        peer = (ka + k) % KA
        return pltpu.make_async_remote_copy(
            src_ref=sums.at[peer % 2], dst_ref=means.at[ka], send_sem=mean_s.at[k],
            recv_sem=mean_r.at[ka], device_id={"ka": peer}, device_id_type=MESH,
        )

    def mean_arrival(k):
        peer = (ka + k) % KA
        return pltpu.make_async_remote_copy(
            src_ref=sums.at[c], dst_ref=means.at[peer], send_sem=mean_s.at[k],
            recv_sem=mean_r.at[peer], device_id={"ka": peer}, device_id_type=MESH,
        )

    swap = pltpu.make_async_remote_copy(
        src_ref=deq.at[other], dst_ref=kv_full.at[:, own_rows], send_sem=kvx_s, recv_sem=kvx_r,
        device_id={"ka": sibling}, device_id_type=MESH,
    )
    their_rows = pl.ds(pl.multiple_of(KEYS * other, KEYS), KEYS)
    swapped = pltpu.make_async_remote_copy(
        src_ref=deq.at[other], dst_ref=kv_full.at[:, their_rows], send_sem=kvx_s, recv_sem=kvx_r,
        device_id={"ka": sibling}, device_id_type=MESH,
    )
    for k in FAR_FIRST:
        mean_copy(k).start()
    swap.start()
    swapped.wait_recv()

    lanes = lax.broadcasted_iota(jnp.int32, (CKEYS, D), 1)
    k_ones = jnp.where(lanes < 3 * GROUP, -1.0, 0.0).astype(BF16)
    v_ones = jnp.where((lanes >= 3 * GROUP) & (lanes < 6 * GROUP), -1.0, 0.0).astype(BF16)

    kt[0:D, :] = kv_full[0].astype(F32).T.astype(BF16)
    kt[D:, :] = jnp.ones((16, CKEYS), BF16)
    token = lax.shift_right_logical(lax.broadcasted_iota(jnp.int32, (16, ROWS), 1), 3)
    gap = lax.broadcasted_iota(jnp.int32, (16, ROWS), 0) - token

    def first(i, carry):
        places = []
        for at in range(2):
            s = 2 * i + at
            places.append((at, s, pl.ds(pl.multiple_of(s * ROWS, ROWS), ROWS)))
        for at, s, rows in places:
            extra = mbuf[rows, :]
            k_in = jnp.concatenate([kv_full[0], k_ones], axis=1)
            v_in = jnp.concatenate([kv_full[1], v_ones], axis=1)
            s_all[s] = dot(k_in, jnp.concatenate([q2[rows, :], extra], axis=1), NT)
            dp_all[s] = dot(v_in, jnp.concatenate([go2[rows, :], extra], axis=1), NT)
        for at, s, rows in places:
            limit = TOK * b + SHARE * s - CKEYS * z
            top = jnp.full((16, ROWS), HIDDEN, F32)
            for k0 in range(0, CKEYS, 16):
                a = jnp.where(gap + k0 <= limit, s_all[s, k0:k0 + 16, :] * (inv * LOG2E), HIDDEN)
                s_all[s, k0:k0 + 16, :] = a
                top = jnp.maximum(top, a)
            peak = jnp.max(top, axis=0, keepdims=True)
            stab[s] = peak
            for k0 in range(0, CKEYS, 16):
                w = jnp.exp2(s_all[s, k0:k0 + 16, :] - peak)
                f = w * dp_all[s, k0:k0 + 16, :]
                s_all[s, k0:k0 + 16, :] = w
                dp_all[s, k0:k0 + 16, :] = f
                ds_scr[at, k0:k0 + 16, :] = f.astype(BF16)
        for at, s, rows in places:
            both_sums = dot(kt[...], ds_scr[at], NN)
            dqt[s] = both_sums[0:D]
            totf[s] = both_sums[D:D + 1]
        return carry

    lax.fori_loop(0, NZ // 2, first, 0)

    m_row = lax.broadcasted_iota(jnp.int32, (2 * KEYS, KEYS), 0)
    m_col = lax.broadcasted_iota(jnp.int32, (2 * KEYS, KEYS), 1)
    for h in range(2):
        merge[h] = jnp.where(m_row == 2 * m_col + h, 1.0, 0.0).astype(BF16)

    for k in range(1, KA):
        mean_arrival(k).wait_recv()
    means[ka] = sums[c]
    total = means[0]
    for k in range(1, KA):
        total = total + means[k]
    mean = jnp.broadcast_to(total / (KA * KEYS), (8, D))
    mean_col = jnp.broadcast_to(mean[0:1], (D, D)).T
    m_hi, m_mid, m_lo = split3(mean)
    srow = lax.broadcasted_iota(jnp.int32, (8, D), 0)
    mean_rows = jnp.where(srow == 0, m_hi, jnp.where(srow == 1, m_mid, jnp.where(srow == 2, m_lo, 0.0)))
    mean_rows = jnp.concatenate([mean_rows, jnp.zeros((8, D), F32)], axis=0).astype(BF16)
    acc[...] = jnp.zeros_like(acc)

    def offset(t):
        return jnp.where(t % 2 == 1, (t - 1) // 2 - 3, NZ // 2 - t // 2)

    left = (z + NZ - 1) % NZ
    right = (z + 1) % NZ

    def hop(t, half):
        leftward = half == 0 if t == 0 else t % 2 == 1
        to = left if leftward else right
        if t < 5:
            at = (1 if half == 0 else 2) if t == 0 else t + 2
            return pltpu.make_async_remote_copy(
                src_ref=tx.at[t, half], dst_ref=rx.at[at, half], send_sem=tx_s.at[t, half],
                recv_sem=rx_r.at[at, half], device_id={"ka": 2 * to + c}, device_id_type=MESH,
            )
        side = 0 if leftward else 1
        return pltpu.make_async_remote_copy(
            src_ref=tx.at[t, half], dst_ref=fin.at[side, c], send_sem=tx_s.at[t, half],
            recv_sem=fin_r.at[side, c], device_id={"ka": 2 * to + half}, device_id_type=MESH,
        )

    def arrival(t, half):
        return pltpu.make_async_remote_copy(
            src_ref=tx.at[t, half], dst_ref=rx.at[t, half], send_sem=tx_s.at[t, half],
            recv_sem=rx_r.at[t, half], device_id={"ka": sibling}, device_id_type=MESH,
        )

    def part(t, half):
        return dqbuf[t, half * HALF:(half + 1) * HALF, :]

    def begin(t, half):
        tx[t, half] = part(t, half).astype(BF16)
        hop(t, half).start()

    def forward(t, half):
        arrival(t, half).wait_recv()
        tx[t, half] = (part(t, half) + rx[t, half].astype(F32)).astype(BF16)
        hop(t, half).start()

    def finish_share(t):
        s = (z + offset(t) + NZ) % NZ
        rows = pl.ds(pl.multiple_of(s * ROWS, ROWS), ROWS)
        shift = jnp.sum(dot(mean_rows, q2[rows, :], NT)[0:8], axis=0, keepdims=True)
        factor = jnp.exp2(stab[s] - shift * (inv * LOG2E))
        gain[s] = factor
        for l0 in range(0, ROWS, D):
            at = slice(l0, l0 + D)
            centred = dqt[s, :, at] - mean_col * totf[s, :, at]
            dqbuf[t, at, :] = (centred * (factor[:, at] * inv)).T

    for t in range(NZ):
        finish_share(t)
        if t == 0:
            begin(0, 0)
            begin(0, 1)
        elif t == 1:
            begin(1, 1)
        elif t == 2:
            begin(2, 0)

    def second(i, carry):
        places = []
        for at in range(2):
            s = 2 * i + at
            places.append((at, s, pl.ds(pl.multiple_of(s * ROWS, ROWS), ROWS)))
        for at, s, rows in places:
            factor = gain[s]
            for k0 in range(0, CKEYS, 16):
                p_scr[at, k0:k0 + 16, :] = (s_all[s, k0:k0 + 16, :] * factor).astype(BF16)
                ds_scr[at, k0:k0 + 16, :] = (dp_all[s, k0:k0 + 16, :] * factor).astype(BF16)
        add_k, add_v = acc[0], acc[1]
        for at, s, rows in places:
            add_k = add_k + dot(ds_scr[at], q2[rows, :], NN)
            add_v = add_v + dot(p_scr[at], go2[rows, :], NN)
        acc[0] = add_k
        acc[1] = add_v
        return carry

    lax.fori_loop(0, NZ // 2, second, 0)

    kvtx[0] = (acc[0] * inv).astype(BF16)
    kvtx[1] = acc[1].astype(BF16)

    def piece_copy(k):
        peer = (b + k) % PB
        return pltpu.make_async_remote_copy(
            src_ref=kvtx.at[:, pl.ds(pl.multiple_of(peer * PIECE, PIECE), PIECE)], dst_ref=kvrx.at[b],
            send_sem=pb_s.at[k], recv_sem=pb_r.at[b], device_id={"pb": peer}, device_id_type=MESH,
        )

    def piece_arrival(k):
        peer = (b + k) % PB
        return pltpu.make_async_remote_copy(
            src_ref=kvtx.at[:, pl.ds(pl.multiple_of(peer * PIECE, PIECE), PIECE)], dst_ref=kvrx.at[peer],
            send_sem=pb_s.at[k], recv_sem=pb_r.at[peer], device_id={"pb": peer}, device_id_type=MESH,
        )

    for k in range(1, PB):
        piece_copy(k).start()

    tx[7, 0] = part(7, 0).astype(BF16)
    tx[7, 1] = part(7, 1).astype(BF16)
    to_sib = pltpu.make_async_remote_copy(
        src_ref=tx.at[7, other], dst_ref=sib, send_sem=tx_s.at[7, 0], recv_sem=sib_r,
        device_id={"ka": sibling}, device_id_type=MESH,
    )
    to_sib.start()

    forward(1, 0)
    forward(2, 1)
    for t in (3, 4, 5, 6):
        for half in range(2):
            forward(t, half)

    for k in range(1, PB):
        piece_arrival(k).wait_recv()
    kvrx[b] = kvtx[:, pl.ds(pl.multiple_of(b * PIECE, PIECE), PIECE), :]
    gathered = kvrx[0].astype(F32)
    for k in range(1, PB):
        gathered = gathered + kvrx[k].astype(F32)
    red[...] = gathered.astype(BF16)

    owner = b // (PB // 2)
    slot = b % (PB // 2)
    goal = ag.at[:, c, pl.ds(pl.multiple_of(slot * PIECE, PIECE), PIECE)]

    def spread_copy(k):
        return pltpu.make_async_remote_copy(
            src_ref=red, dst_ref=goal, send_sem=ag_s.at[k], recv_sem=ag_r.at[c, slot],
            device_id={"pb": (b + k) % PB, "ka": 2 * z + owner}, device_id_type=MESH,
        )

    def spread_arrival(h, sl):
        return pltpu.make_async_remote_copy(
            src_ref=red, dst_ref=ag.at[:, h, pl.ds(sl * PIECE, PIECE)], send_sem=ag_s.at[0],
            recv_sem=ag_r.at[h, sl], device_id={"ka": sibling}, device_id_type=MESH,
        )

    for k in range(1, PB):
        spread_copy(k).start()

    @pl.when(owner == c)
    def _():
        ag[:, c, pl.ds(pl.multiple_of(slot * PIECE, PIECE), PIECE), :] = red[...]

    @pl.when(owner != c)
    def _():
        spread_copy(0).start()

    for side in range(2):
        for h in range(2):
            pltpu.make_async_remote_copy(
                src_ref=tx.at[5, 0], dst_ref=fin.at[side, h], send_sem=tx_s.at[5, 0],
                recv_sem=fin_r.at[side, h], device_id={"ka": sibling}, device_id_type=MESH,
            ).wait_recv()
    to_sib.wait_recv()
    mine = dqbuf[7, pl.ds(pl.multiple_of(c * HALF, HALF), HALF), :]
    for h, local in ((c, mine), (other, sib[...].astype(F32))):
        whole = local + fin[0, h].astype(F32) + fin[1, h].astype(F32)
        dq_ref[:, h] = whole.reshape(HALF // GROUP, GROUP, D).astype(BF16)

    for h in range(2):
        for sl in range(PB // 2):
            @pl.when(jnp.logical_not((owner == c) & (slot == sl) & (c == h)))
            def _():
                spread_arrival(h, sl).wait_recv()
    side_by_side = [jnp.concatenate([ag[0, h], ag[1, h]], axis=1) for h in range(2)]
    merged = dot(merge[0], side_by_side[0], NN) + dot(merge[1], side_by_side[1], NN)
    dkv_ref[0] = merged[:, :D].astype(BF16)
    dkv_ref[1] = merged[:, D:].astype(BF16)

    for k in range(1, KA):
        mean_copy(k).wait_send()
    swap.wait_send()
    for t in range(7):
        for half in range(2):
            hop(t, half).wait_send()
    to_sib.wait_send()
    for k in range(1, PB):
        piece_copy(k).wait_send()
        spread_copy(k).wait_send()

    @pl.when(owner != c)
    def _():
        spread_copy(0).wait_send()


def write_out(dq_ref, dkv_ref, dq_hbm, dk_hbm, dv_hbm, sems):
    copies = [
        pltpu.make_async_copy(dq_ref, dq_hbm, sems.at[0]),
        pltpu.make_async_copy(dkv_ref.at[0], dk_hbm, sems.at[1]),
        pltpu.make_async_copy(dkv_ref.at[1], dv_hbm, sems.at[2]),
    ]
    for copy in copies:
        copy.start()
    for copy in copies:
        copy.wait()


def per_device(queries, key_codes, key_scale_powers, values, grad_out, grad_dot, log_totals):
    vmem = pl.BlockSpec(memory_space=pltpu.VMEM)
    anyw = pl.BlockSpec(memory_space=pl.ANY)
    dma = pltpu.SemaphoreType.DMA
    dq, dkv = pl.pallas_call(
        kernel,
        out_shape=(
            pltpu.VMEM((TOK // KA, 2, GROUP, D), BF16),
            pltpu.VMEM((2, 2 * KEYS, D), BF16),
        ),
        in_specs=[anyw] * 7,
        out_specs=(vmem, vmem),
        scratch_shapes=[
            pltpu.VMEM((GROUP, TOK), F32),
            pltpu.VMEM((GROUP, TOK), F32),
            pltpu.VMEM((2 * KEYS, D), BF16),
            pltpu.VMEM((2 * KEYS, D), BF16),
            pltpu.SMEM((2, KEYS // KEYS_PER_SCALE), jnp.int32),
            pltpu.VMEM((2, 2 * KEYS, KEYS), BF16),
            pltpu.VMEM((TOK, GROUP, D), BF16),
            pltpu.VMEM((TOK, GROUP, D), BF16),
            pltpu.VMEM((TOK * GROUP, D), BF16),
            pltpu.VMEM((TOK * GROUP, D), BF16),
            pltpu.VMEM((TOK * GROUP, D), BF16),
            pltpu.VMEM((2, 2, KEYS, D), BF16),
            pltpu.VMEM((2, CKEYS, D), BF16),
            pltpu.VMEM((2, 1, D), F32),
            pltpu.VMEM((KA, 1, D), F32),
            pltpu.VMEM((D + 16, CKEYS), BF16),
            pltpu.VMEM((NZ, CKEYS, ROWS), F32),
            pltpu.VMEM((NZ, CKEYS, ROWS), F32),
            pltpu.VMEM((NZ, 1, ROWS), F32),
            pltpu.VMEM((NZ, 1, ROWS), F32),
            pltpu.VMEM((NZ, 1, ROWS), F32),
            pltpu.VMEM((NZ, D, ROWS), F32),
            pltpu.VMEM((2, CKEYS, ROWS), BF16),
            pltpu.VMEM((2, CKEYS, ROWS), BF16),
            pltpu.VMEM((NZ, ROWS, D), F32),
            pltpu.VMEM((2, CKEYS, D), F32),
            pltpu.VMEM((NZ, 2, HALF, D), BF16),
            pltpu.VMEM((7, 2, HALF, D), BF16),
            pltpu.VMEM((2, 2, HALF, D), BF16),
            pltpu.VMEM((HALF, D), BF16),
            pltpu.VMEM((2, CKEYS, D), BF16),
            pltpu.VMEM((PB, 2, PIECE, D), BF16),
            pltpu.VMEM((2, PIECE, D), BF16),
            pltpu.VMEM((2, 2, KEYS, D), BF16),
            dma((7,)),
            dma,
            dma,
            dma((KA,)),
            dma((KA,)),
            dma((NZ, 2)),
            dma((7, 2)),
            dma((2, 2)),
            dma,
            dma((PB,)),
            dma((PB,)),
            dma((PB,)),
            dma((2, PB // 2)),
        ],
        compiler_params=pltpu.CompilerParams(collective_id=0, has_side_effects=True),
    )(
        queries.reshape(TOK, 2, GROUP, D),
        grad_out.reshape(TOK, 2, GROUP, D),
        log_totals.T,
        grad_dot.T,
        key_codes.reshape(2 * KEYS, D),
        values.reshape(2 * KEYS, D),
        key_scale_powers.T,
    )
    dq, dk, dv = pl.pallas_call(
        write_out,
        out_shape=(
            jax.ShapeDtypeStruct((TOK // KA, 2, GROUP, D), BF16),
            jax.ShapeDtypeStruct((2 * KEYS, D), BF16),
            jax.ShapeDtypeStruct((2 * KEYS, D), BF16),
        ),
        in_specs=[vmem, vmem],
        out_specs=(anyw, anyw, anyw),
        scratch_shapes=[dma((3,))],
        compiler_params=pltpu.CompilerParams(vmem_limit_bytes=4 * 1024 * 1024),
    )(dq, dkv)
    return (
        dq.reshape(TOK // KA, 2 * GROUP, D),
        dk.reshape(KEYS, 2, D),
        dv.reshape(KEYS, 2, D),
    )


def solution(mesh):
    in_specs = (
        P("pb", "ha", None),
        P("ka", "ha", None),
        P("ka", "ha"),
        P("ka", "ha", None),
        P("pb", "ha", None),
        P("pb", "ha"),
        P("pb", "ha"),
    )
    out_specs = (P(("pb", "ka"), "ha", None), P("ka", "ha", None), P("ka", "ha", None))
    return jax.shard_map(
        per_device, mesh=mesh, in_specs=in_specs, out_specs=out_specs, check_vma=False
    )
```

```python
import functools

import jax
import jax.numpy as jnp
from jax import lax
from jax.experimental import pallas as pl
from jax.experimental.pallas import tpu as pltpu
from jax.sharding import PartitionSpec as P

F32 = jnp.float32
BF16 = jnp.bfloat16
MESH = pl.DeviceIdType.MESH
NT = (((1,), (1,)), ((), ()))
NN = (((1,), (0,)), ((), ()))

PB = 8
NZ = 8
KA = 16
TOK = 384
GROUP = 8
D = 128
KEYS = 192
CKEYS = 384
SHARE = 48
ROWS = SHARE * GROUP
HALF = ROWS // 2
PIECE = CKEYS // PB
KEYS_PER_SCALE = 64
LOG2E = 1.4426950408889634
HIDDEN = -1e30
FAR_FIRST = sorted(range(1, KA), key=lambda k: (abs(k - KA // 2), k))


def dot(a, b, dims):
    return lax.dot_general(a, b, dims, preferred_element_type=F32)


def split3(x):
    hi = x.astype(BF16).astype(F32)
    rest = x - hi
    mid = rest.astype(BF16).astype(F32)
    return hi, mid, rest - mid


def kernel(
    q_hbm, go_hbm, tot_hbm, dots_hbm, codes_hbm, vals_hbm, pows_hbm,
    dq_ref, dkv_ref,
    tot_ref, dots_ref, codes_ref, vals_ref, pows_ref, merge,
    qbuf, gobuf, q2, go2, mbuf, deq, kv_full, sums, means, kt, s_all, dp_all,
    stab, totf, gain, dqt, p_scr, ds_scr, dqbuf, acc, tx, rx, fin, sib, kvtx, kvrx, red, ag,
    in_sem, kvx_s, kvx_r, mean_s, mean_r, tx_s, rx_r, fin_r, sib_r,
    pb_s, pb_r, ag_s, ag_r,
):
    b = lax.axis_index("pb")
    ka = lax.axis_index("ka")
    z = ka // 2
    c = ka % 2
    other = 1 - c
    sibling = 2 * z + other
    inv = D ** -0.5

    barrier = pltpu.get_barrier_semaphore()
    for k in FAR_FIRST:
        pl.semaphore_signal(barrier, inc=1, device_id={"ka": (ka + k) % KA}, device_id_type=MESH)
    for k in range(1, PB):
        for core in range(2):
            pl.semaphore_signal(
                barrier, inc=1, device_id={"pb": (b + k) % PB, "ka": 2 * z + core}, device_id_type=MESH
            )

    q_copy = pltpu.make_async_copy(q_hbm.at[:, c], qbuf, in_sem.at[0])
    go_copy = pltpu.make_async_copy(go_hbm.at[:, c], gobuf, in_sem.at[1])
    heads = pl.ds(pl.multiple_of(GROUP * c, GROUP), GROUP)
    loads = [
        pltpu.make_async_copy(codes_hbm, codes_ref, in_sem.at[2]),
        pltpu.make_async_copy(vals_hbm, vals_ref, in_sem.at[3]),
        pltpu.make_async_copy(pows_hbm, pows_ref, in_sem.at[4]),
        pltpu.make_async_copy(tot_hbm.at[heads], tot_ref, in_sem.at[5]),
        pltpu.make_async_copy(dots_hbm.at[heads], dots_ref, in_sem.at[6]),
    ]
    for load in loads:
        load.start()
    q_copy.start()
    go_copy.start()
    for load in loads:
        load.wait()

    both = jnp.concatenate([codes_ref[...], vals_ref[...]], axis=1)
    for h in range(2):
        row = lax.broadcasted_iota(jnp.int32, (KEYS, 2 * KEYS), 0)
        col = lax.broadcasted_iota(jnp.int32, (KEYS, 2 * KEYS), 1)
        pick = jnp.where(col == 2 * row + h, 1.0, 0.0).astype(BF16)
        picked = dot(pick, both, NN)
        total = jnp.zeros((1, D), F32)
        for blk in range(KEYS // KEYS_PER_SCALE):
            at = slice(blk * KEYS_PER_SCALE, (blk + 1) * KEYS_PER_SCALE)
            power = jnp.full((KEYS_PER_SCALE, D), pows_ref[h, blk], jnp.int32).astype(F32)
            scaled = picked[at, :D] * jnp.exp2(power)
            total = total + jnp.sum(scaled, axis=0, keepdims=True)
            deq[h, 0, at, :] = scaled.astype(BF16)
        deq[h, 1, :, :] = picked[:, D:].astype(BF16)
        sums[h] = total

    own_rows = pl.ds(pl.multiple_of(KEYS * c, KEYS), KEYS)
    kv_full[:, own_rows, :] = deq[c]

    pieces = split3(tot_ref[...] * (D ** 0.5)) + split3(dots_ref[...])
    stacked = jnp.concatenate(list(pieces) + [jnp.zeros((D - 6 * GROUP, TOK), F32)], axis=0)
    by_token = stacked.T
    lane = lax.broadcasted_iota(jnp.int32, (GROUP, D), 1)
    sub = lax.broadcasted_iota(jnp.int32, (GROUP, D), 0)
    own_lane = jnp.where((lane & (GROUP - 1)) == sub, 1.0, 0.0)
    for s in range(NZ):
        at = by_token[s * SHARE:(s + 1) * SHARE]
        spread = at[:, None, :] * own_lane[None]
        mbuf[s * ROWS:(s + 1) * ROWS, :] = spread.reshape(ROWS, D).astype(BF16)

    q_copy.wait()
    go_copy.wait()

    def flatten(s, carry):
        toks = pl.ds(s * SHARE, SHARE)
        rows = pl.ds(pl.multiple_of(s * ROWS, ROWS), ROWS)
        q2[rows, :] = qbuf[toks].astype(F32).reshape(ROWS, D).astype(BF16)
        go2[rows, :] = gobuf[toks].astype(F32).reshape(ROWS, D).astype(BF16)
        return carry

    lax.fori_loop(0, NZ, flatten, 0)

    pl.semaphore_wait(barrier, KA - 1 + 2 * (PB - 1))

    def mean_copy(k):
        peer = (ka + k) % KA
        return pltpu.make_async_remote_copy(
            src_ref=sums.at[peer % 2], dst_ref=means.at[ka], send_sem=mean_s.at[k],
            recv_sem=mean_r.at[ka], device_id={"ka": peer}, device_id_type=MESH,
        )

    def mean_arrival(k):
        peer = (ka + k) % KA
        return pltpu.make_async_remote_copy(
            src_ref=sums.at[c], dst_ref=means.at[peer], send_sem=mean_s.at[k],
            recv_sem=mean_r.at[peer], device_id={"ka": peer}, device_id_type=MESH,
        )

    swap = pltpu.make_async_remote_copy(
        src_ref=deq.at[other], dst_ref=kv_full.at[:, own_rows], send_sem=kvx_s, recv_sem=kvx_r,
        device_id={"ka": sibling}, device_id_type=MESH,
    )
    their_rows = pl.ds(pl.multiple_of(KEYS * other, KEYS), KEYS)
    swapped = pltpu.make_async_remote_copy(
        src_ref=deq.at[other], dst_ref=kv_full.at[:, their_rows], send_sem=kvx_s, recv_sem=kvx_r,
        device_id={"ka": sibling}, device_id_type=MESH,
    )
    for k in FAR_FIRST:
        mean_copy(k).start()
    swap.start()
    swapped.wait_recv()

    lanes = lax.broadcasted_iota(jnp.int32, (CKEYS, D), 1)
    k_ones = jnp.where(lanes < 3 * GROUP, -1.0, 0.0).astype(BF16)
    v_ones = jnp.where((lanes >= 3 * GROUP) & (lanes < 6 * GROUP), -1.0, 0.0).astype(BF16)

    kt[0:D, :] = kv_full[0].astype(F32).T.astype(BF16)
    kt[D:, :] = jnp.ones((16, CKEYS), BF16)
    token = lax.shift_right_logical(lax.broadcasted_iota(jnp.int32, (16, ROWS), 1), 3)
    gap = lax.broadcasted_iota(jnp.int32, (16, ROWS), 0) - token

    def first(i, carry):
        places = []
        for at in range(2):
            s = 2 * i + at
            places.append((at, s, pl.ds(pl.multiple_of(s * ROWS, ROWS), ROWS)))
        for at, s, rows in places:
            extra = mbuf[rows, :]
            k_in = jnp.concatenate([kv_full[0], k_ones], axis=1)
            v_in = jnp.concatenate([kv_full[1], v_ones], axis=1)
            s_all[s] = dot(k_in, jnp.concatenate([q2[rows, :], extra], axis=1), NT)
            dp_all[s] = dot(v_in, jnp.concatenate([go2[rows, :], extra], axis=1), NT)
        for at, s, rows in places:
            limit = TOK * b + SHARE * s - CKEYS * z
            top = jnp.full((16, ROWS), HIDDEN, F32)
            for k0 in range(0, CKEYS, 16):
                a = jnp.where(gap + k0 <= limit, s_all[s, k0:k0 + 16, :] * (inv * LOG2E), HIDDEN)
                s_all[s, k0:k0 + 16, :] = a
                top = jnp.maximum(top, a)
            peak = jnp.max(top, axis=0, keepdims=True)
            stab[s] = peak
            for k0 in range(0, CKEYS, 16):
                w = jnp.exp2(s_all[s, k0:k0 + 16, :] - peak)
                f = w * dp_all[s, k0:k0 + 16, :]
                s_all[s, k0:k0 + 16, :] = w
                dp_all[s, k0:k0 + 16, :] = f
                ds_scr[at, k0:k0 + 16, :] = f.astype(BF16)
        for at, s, rows in places:
            both_sums = dot(kt[...], ds_scr[at], NN)
            dqt[s] = both_sums[0:D]
            totf[s] = both_sums[D:D + 1]
        return carry

    lax.fori_loop(0, NZ // 2, first, 0)

    m_row = lax.broadcasted_iota(jnp.int32, (2 * KEYS, KEYS), 0)
    m_col = lax.broadcasted_iota(jnp.int32, (2 * KEYS, KEYS), 1)
    for h in range(2):
        merge[h] = jnp.where(m_row == 2 * m_col + h, 1.0, 0.0).astype(BF16)

    for k in range(1, KA):
        mean_arrival(k).wait_recv()
    means[ka] = sums[c]
    total = means[0]
    for k in range(1, KA):
        total = total + means[k]
    mean = jnp.broadcast_to(total / (KA * KEYS), (8, D))
    mean_col = jnp.broadcast_to(mean[0:1], (D, D)).T
    m_hi, m_mid, m_lo = split3(mean)
    srow = lax.broadcasted_iota(jnp.int32, (8, D), 0)
    mean_rows = jnp.where(srow == 0, m_hi, jnp.where(srow == 1, m_mid, jnp.where(srow == 2, m_lo, 0.0)))
    mean_rows = jnp.concatenate([mean_rows, jnp.zeros((8, D), F32)], axis=0).astype(BF16)
    acc[...] = jnp.zeros_like(acc)

    def offset(t):
        return jnp.where(t % 2 == 1, (t - 1) // 2 - 3, NZ // 2 - t // 2)

    left = (z + NZ - 1) % NZ
    right = (z + 1) % NZ

    def hop(t, half):
        leftward = half == 0 if t == 0 else t % 2 == 1
        to = left if leftward else right
        if t < 5:
            at = (1 if half == 0 else 2) if t == 0 else t + 2
            return pltpu.make_async_remote_copy(
                src_ref=tx.at[t, half], dst_ref=rx.at[at, half], send_sem=tx_s.at[t, half],
                recv_sem=rx_r.at[at, half], device_id={"ka": 2 * to + c}, device_id_type=MESH,
            )
        side = 0 if leftward else 1
        return pltpu.make_async_remote_copy(
            src_ref=tx.at[t, half], dst_ref=fin.at[side, c], send_sem=tx_s.at[t, half],
            recv_sem=fin_r.at[side, c], device_id={"ka": 2 * to + half}, device_id_type=MESH,
        )

    def arrival(t, half):
        return pltpu.make_async_remote_copy(
            src_ref=tx.at[t, half], dst_ref=rx.at[t, half], send_sem=tx_s.at[t, half],
            recv_sem=rx_r.at[t, half], device_id={"ka": sibling}, device_id_type=MESH,
        )

    def part(t, half):
        return dqbuf[t, half * HALF:(half + 1) * HALF, :]

    def begin(t, half):
        tx[t, half] = part(t, half).astype(BF16)
        hop(t, half).start()

    def forward(t, half):
        arrival(t, half).wait_recv()
        tx[t, half] = (part(t, half) + rx[t, half].astype(F32)).astype(BF16)
        hop(t, half).start()

    def finish_share(t):
        s = (z + offset(t) + NZ) % NZ
        rows = pl.ds(pl.multiple_of(s * ROWS, ROWS), ROWS)
        shift = jnp.sum(dot(mean_rows, q2[rows, :], NT)[0:8], axis=0, keepdims=True)
        factor = jnp.exp2(stab[s] - shift * (inv * LOG2E))
        gain[s] = factor
        for l0 in range(0, ROWS, D):
            at = slice(l0, l0 + D)
            centred = dqt[s, :, at] - mean_col * totf[s, :, at]
            dqbuf[t, at, :] = (centred * (factor[:, at] * inv)).T

    for t in range(NZ):
        finish_share(t)
        if t == 0:
            begin(0, 0)
            begin(0, 1)
        elif t == 1:
            begin(1, 1)
        elif t == 2:
            begin(2, 0)

    def second(i, carry):
        places = []
        for at in range(2):
            s = 2 * i + at
            places.append((at, s, pl.ds(pl.multiple_of(s * ROWS, ROWS), ROWS)))
        for at, s, rows in places:
            factor = gain[s]
            for k0 in range(0, CKEYS, 16):
                p_scr[at, k0:k0 + 16, :] = (s_all[s, k0:k0 + 16, :] * factor).astype(BF16)
                ds_scr[at, k0:k0 + 16, :] = (dp_all[s, k0:k0 + 16, :] * factor).astype(BF16)
        add_k, add_v = acc[0], acc[1]
        for at, s, rows in places:
            add_k = add_k + dot(ds_scr[at], q2[rows, :], NN)
            add_v = add_v + dot(p_scr[at], go2[rows, :], NN)
        acc[0] = add_k
        acc[1] = add_v
        return carry

    lax.fori_loop(0, NZ // 2, second, 0)

    kvtx[0] = (acc[0] * inv).astype(BF16)
    kvtx[1] = acc[1].astype(BF16)

    def piece_copy(k):
        peer = (b + k) % PB
        return pltpu.make_async_remote_copy(
            src_ref=kvtx.at[:, pl.ds(pl.multiple_of(peer * PIECE, PIECE), PIECE)], dst_ref=kvrx.at[b],
            send_sem=pb_s.at[k], recv_sem=pb_r.at[b], device_id={"pb": peer}, device_id_type=MESH,
        )

    def piece_arrival(k):
        peer = (b + k) % PB
        return pltpu.make_async_remote_copy(
            src_ref=kvtx.at[:, pl.ds(pl.multiple_of(peer * PIECE, PIECE), PIECE)], dst_ref=kvrx.at[peer],
            send_sem=pb_s.at[k], recv_sem=pb_r.at[peer], device_id={"pb": peer}, device_id_type=MESH,
        )

    for k in range(1, PB):
        piece_copy(k).start()

    tx[7, 0] = part(7, 0).astype(BF16)
    tx[7, 1] = part(7, 1).astype(BF16)
    to_sib = pltpu.make_async_remote_copy(
        src_ref=tx.at[7, other], dst_ref=sib, send_sem=tx_s.at[7, 0], recv_sem=sib_r,
        device_id={"ka": sibling}, device_id_type=MESH,
    )
    to_sib.start()

    for which in ((1, 0), (2, 1), (3, 1), (4, 0)):
        forward(*which)
    for which in ((3, 0), (4, 1), (5, 1), (6, 0)):
        forward(*which)

    for k in range(1, PB):
        piece_arrival(k).wait_recv()
    kvrx[b] = kvtx[:, pl.ds(pl.multiple_of(b * PIECE, PIECE), PIECE), :]
    gathered = kvrx[0].astype(F32)
    for k in range(1, PB):
        gathered = gathered + kvrx[k].astype(F32)
    red[...] = gathered.astype(BF16)

    owner = b // (PB // 2)
    slot = b % (PB // 2)
    goal = ag.at[:, c, pl.ds(pl.multiple_of(slot * PIECE, PIECE), PIECE)]

    def spread_copy(k):
        return pltpu.make_async_remote_copy(
            src_ref=red, dst_ref=goal, send_sem=ag_s.at[k], recv_sem=ag_r.at[c, slot],
            device_id={"pb": (b + k) % PB, "ka": 2 * z + owner}, device_id_type=MESH,
        )

    def spread_arrival(h, sl):
        return pltpu.make_async_remote_copy(
            src_ref=red, dst_ref=ag.at[:, h, pl.ds(sl * PIECE, PIECE)], send_sem=ag_s.at[0],
            recv_sem=ag_r.at[h, sl], device_id={"ka": sibling}, device_id_type=MESH,
        )

    for k in range(1, PB):
        spread_copy(k).start()

    @pl.when(owner == c)
    def _():
        ag[:, c, pl.ds(pl.multiple_of(slot * PIECE, PIECE), PIECE), :] = red[...]

    @pl.when(owner != c)
    def _():
        spread_copy(0).start()

    for which in ((5, 0), (6, 1)):
        forward(*which)

    for side in range(2):
        for h in range(2):
            pltpu.make_async_remote_copy(
                src_ref=tx.at[5, 0], dst_ref=fin.at[side, h], send_sem=tx_s.at[5, 0],
                recv_sem=fin_r.at[side, h], device_id={"ka": sibling}, device_id_type=MESH,
            ).wait_recv()
    to_sib.wait_recv()
    mine = dqbuf[7, pl.ds(pl.multiple_of(c * HALF, HALF), HALF), :]
    for h, local in ((c, mine), (other, sib[...].astype(F32))):
        whole = local + fin[0, h].astype(F32) + fin[1, h].astype(F32)
        dq_ref[:, h] = whole.reshape(HALF // GROUP, GROUP, D).astype(BF16)

    for h in range(2):
        for sl in range(PB // 2):
            @pl.when(jnp.logical_not((owner == c) & (slot == sl) & (c == h)))
            def _():
                spread_arrival(h, sl).wait_recv()
    side_by_side = [jnp.concatenate([ag[0, h], ag[1, h]], axis=1) for h in range(2)]
    merged = dot(merge[0], side_by_side[0], NN) + dot(merge[1], side_by_side[1], NN)
    dkv_ref[0] = merged[:, :D].astype(BF16)
    dkv_ref[1] = merged[:, D:].astype(BF16)

    for k in range(1, KA):
        mean_copy(k).wait_send()
    swap.wait_send()
    for t in range(7):
        for half in range(2):
            hop(t, half).wait_send()
    to_sib.wait_send()
    for k in range(1, PB):
        piece_copy(k).wait_send()
        spread_copy(k).wait_send()

    @pl.when(owner != c)
    def _():
        spread_copy(0).wait_send()


def write_out(dq_ref, dkv_ref, dq_hbm, dk_hbm, dv_hbm, sems):
    copies = [
        pltpu.make_async_copy(dq_ref, dq_hbm, sems.at[0]),
        pltpu.make_async_copy(dkv_ref.at[0], dk_hbm, sems.at[1]),
        pltpu.make_async_copy(dkv_ref.at[1], dv_hbm, sems.at[2]),
    ]
    for copy in copies:
        copy.start()
    for copy in copies:
        copy.wait()


def per_device(queries, key_codes, key_scale_powers, values, grad_out, grad_dot, log_totals):
    vmem = pl.BlockSpec(memory_space=pltpu.VMEM)
    anyw = pl.BlockSpec(memory_space=pl.ANY)
    dma = pltpu.SemaphoreType.DMA
    dq, dkv = pl.pallas_call(
        kernel,
        out_shape=(
            pltpu.VMEM((TOK // KA, 2, GROUP, D), BF16),
            pltpu.VMEM((2, 2 * KEYS, D), BF16),
        ),
        in_specs=[anyw] * 7,
        out_specs=(vmem, vmem),
        scratch_shapes=[
            pltpu.VMEM((GROUP, TOK), F32),
            pltpu.VMEM((GROUP, TOK), F32),
            pltpu.VMEM((2 * KEYS, D), BF16),
            pltpu.VMEM((2 * KEYS, D), BF16),
            pltpu.SMEM((2, KEYS // KEYS_PER_SCALE), jnp.int32),
            pltpu.VMEM((2, 2 * KEYS, KEYS), BF16),
            pltpu.VMEM((TOK, GROUP, D), BF16),
            pltpu.VMEM((TOK, GROUP, D), BF16),
            pltpu.VMEM((TOK * GROUP, D), BF16),
            pltpu.VMEM((TOK * GROUP, D), BF16),
            pltpu.VMEM((TOK * GROUP, D), BF16),
            pltpu.VMEM((2, 2, KEYS, D), BF16),
            pltpu.VMEM((2, CKEYS, D), BF16),
            pltpu.VMEM((2, 1, D), F32),
            pltpu.VMEM((KA, 1, D), F32),
            pltpu.VMEM((D + 16, CKEYS), BF16),
            pltpu.VMEM((NZ, CKEYS, ROWS), F32),
            pltpu.VMEM((NZ, CKEYS, ROWS), F32),
            pltpu.VMEM((NZ, 1, ROWS), F32),
            pltpu.VMEM((NZ, 1, ROWS), F32),
            pltpu.VMEM((NZ, 1, ROWS), F32),
            pltpu.VMEM((NZ, D, ROWS), F32),
            pltpu.VMEM((2, CKEYS, ROWS), BF16),
            pltpu.VMEM((2, CKEYS, ROWS), BF16),
            pltpu.VMEM((NZ, ROWS, D), F32),
            pltpu.VMEM((2, CKEYS, D), F32),
            pltpu.VMEM((NZ, 2, HALF, D), BF16),
            pltpu.VMEM((7, 2, HALF, D), BF16),
            pltpu.VMEM((2, 2, HALF, D), BF16),
            pltpu.VMEM((HALF, D), BF16),
            pltpu.VMEM((2, CKEYS, D), BF16),
            pltpu.VMEM((PB, 2, PIECE, D), BF16),
            pltpu.VMEM((2, PIECE, D), BF16),
            pltpu.VMEM((2, 2, KEYS, D), BF16),
            dma((7,)),
            dma,
            dma,
            dma((KA,)),
            dma((KA,)),
            dma((NZ, 2)),
            dma((7, 2)),
            dma((2, 2)),
            dma,
            dma((PB,)),
            dma((PB,)),
            dma((PB,)),
            dma((2, PB // 2)),
        ],
        compiler_params=pltpu.CompilerParams(collective_id=0, has_side_effects=True),
    )(
        queries.reshape(TOK, 2, GROUP, D),
        grad_out.reshape(TOK, 2, GROUP, D),
        log_totals.T,
        grad_dot.T,
        key_codes.reshape(2 * KEYS, D),
        values.reshape(2 * KEYS, D),
        key_scale_powers.T,
    )
    dq, dk, dv = pl.pallas_call(
        write_out,
        out_shape=(
            jax.ShapeDtypeStruct((TOK // KA, 2, GROUP, D), BF16),
            jax.ShapeDtypeStruct((2 * KEYS, D), BF16),
            jax.ShapeDtypeStruct((2 * KEYS, D), BF16),
        ),
        in_specs=[vmem, vmem],
        out_specs=(anyw, anyw, anyw),
        scratch_shapes=[dma((3,))],
        compiler_params=pltpu.CompilerParams(vmem_limit_bytes=4 * 1024 * 1024),
    )(dq, dkv)
    return (
        dq.reshape(TOK // KA, 2 * GROUP, D),
        dk.reshape(KEYS, 2, D),
        dv.reshape(KEYS, 2, D),
    )


def solution(mesh):
    in_specs = (
        P("pb", "ha", None),
        P("ka", "ha", None),
        P("ka", "ha"),
        P("ka", "ha", None),
        P("pb", "ha", None),
        P("pb", "ha"),
        P("pb", "ha"),
    )
    out_specs = (P(("pb", "ka"), "ha", None), P("ka", "ha", None), P("ka", "ha", None))
    return jax.shard_map(
        per_device, mesh=mesh, in_specs=in_specs, out_specs=out_specs, check_vma=False
    )
```

```python
import functools

import jax
import jax.numpy as jnp
from jax import lax
from jax.experimental import pallas as pl
from jax.experimental.pallas import tpu as pltpu
from jax.sharding import PartitionSpec as P

F32 = jnp.float32
BF16 = jnp.bfloat16
MESH = pl.DeviceIdType.MESH
NT = (((1,), (1,)), ((), ()))
NN = (((1,), (0,)), ((), ()))

PB = 8
NZ = 8
KA = 16
TOK = 384
GROUP = 8
D = 128
KEYS = 192
CKEYS = 384
SHARE = 48
ROWS = SHARE * GROUP
HALF = ROWS // 2
PIECE = CKEYS // PB
KEYS_PER_SCALE = 64
LOG2E = 1.4426950408889634
HIDDEN = -1e30
FAR_FIRST = sorted(range(1, KA), key=lambda k: (abs(k - KA // 2), k))


def dot(a, b, dims):
    return lax.dot_general(a, b, dims, preferred_element_type=F32)


def split3(x):
    hi = x.astype(BF16).astype(F32)
    rest = x - hi
    mid = rest.astype(BF16).astype(F32)
    return hi, mid, rest - mid


def kernel(
    q_hbm, go_hbm, tot_hbm, dots_hbm, codes_hbm, vals_hbm, pows_hbm,
    dq_ref, dkv_ref,
    tot_ref, dots_ref, codes_ref, vals_ref, pows_ref, merge,
    qbuf, gobuf, q2, go2, mbuf, deq, kv_full, sums, means, kt, s_all, dp_all,
    stab, totf, gain, dqt, p_scr, ds_scr, dqbuf, acc, tx, rx, far, fin, sib, kvtx, kvrx, red, ag,
    in_sem, kvx_s, kvx_r, mean_s, mean_r, tx_s, rx_r, far_r, fin_r, sib_r,
    pb_s, pb_r, ag_s, ag_r,
):
    b = lax.axis_index("pb")
    ka = lax.axis_index("ka")
    z = ka // 2
    c = ka % 2
    other = 1 - c
    sibling = 2 * z + other
    inv = D ** -0.5

    barrier = pltpu.get_barrier_semaphore()
    for k in FAR_FIRST:
        pl.semaphore_signal(barrier, inc=1, device_id={"ka": (ka + k) % KA}, device_id_type=MESH)
    for k in range(1, PB):
        for core in range(2):
            pl.semaphore_signal(
                barrier, inc=1, device_id={"pb": (b + k) % PB, "ka": 2 * z + core}, device_id_type=MESH
            )

    q_copy = pltpu.make_async_copy(q_hbm.at[:, c], qbuf, in_sem.at[0])
    go_copy = pltpu.make_async_copy(go_hbm.at[:, c], gobuf, in_sem.at[1])
    heads = pl.ds(pl.multiple_of(GROUP * c, GROUP), GROUP)
    loads = [
        pltpu.make_async_copy(codes_hbm, codes_ref, in_sem.at[2]),
        pltpu.make_async_copy(vals_hbm, vals_ref, in_sem.at[3]),
        pltpu.make_async_copy(pows_hbm, pows_ref, in_sem.at[4]),
        pltpu.make_async_copy(tot_hbm.at[heads], tot_ref, in_sem.at[5]),
        pltpu.make_async_copy(dots_hbm.at[heads], dots_ref, in_sem.at[6]),
    ]
    for load in loads:
        load.start()
    q_copy.start()
    go_copy.start()
    for load in loads:
        load.wait()

    both = jnp.concatenate([codes_ref[...], vals_ref[...]], axis=1)
    for h in range(2):
        row = lax.broadcasted_iota(jnp.int32, (KEYS, 2 * KEYS), 0)
        col = lax.broadcasted_iota(jnp.int32, (KEYS, 2 * KEYS), 1)
        pick = jnp.where(col == 2 * row + h, 1.0, 0.0).astype(BF16)
        picked = dot(pick, both, NN)
        total = jnp.zeros((1, D), F32)
        for blk in range(KEYS // KEYS_PER_SCALE):
            at = slice(blk * KEYS_PER_SCALE, (blk + 1) * KEYS_PER_SCALE)
            power = jnp.full((KEYS_PER_SCALE, D), pows_ref[h, blk], jnp.int32).astype(F32)
            scaled = picked[at, :D] * jnp.exp2(power)
            total = total + jnp.sum(scaled, axis=0, keepdims=True)
            deq[h, 0, at, :] = scaled.astype(BF16)
        deq[h, 1, :, :] = picked[:, D:].astype(BF16)
        sums[h] = total

    own_rows = pl.ds(pl.multiple_of(KEYS * c, KEYS), KEYS)
    kv_full[:, own_rows, :] = deq[c]

    pieces = split3(tot_ref[...] * (D ** 0.5)) + split3(dots_ref[...])
    stacked = jnp.concatenate(list(pieces) + [jnp.zeros((D - 6 * GROUP, TOK), F32)], axis=0)
    by_token = stacked.T
    lane = lax.broadcasted_iota(jnp.int32, (GROUP, D), 1)
    sub = lax.broadcasted_iota(jnp.int32, (GROUP, D), 0)
    own_lane = jnp.where((lane & (GROUP - 1)) == sub, 1.0, 0.0)
    for s in range(NZ):
        at = by_token[s * SHARE:(s + 1) * SHARE]
        spread = at[:, None, :] * own_lane[None]
        mbuf[s * ROWS:(s + 1) * ROWS, :] = spread.reshape(ROWS, D).astype(BF16)

    q_copy.wait()
    go_copy.wait()

    def flatten(s, carry):
        toks = pl.ds(s * SHARE, SHARE)
        rows = pl.ds(pl.multiple_of(s * ROWS, ROWS), ROWS)
        q2[rows, :] = qbuf[toks].astype(F32).reshape(ROWS, D).astype(BF16)
        go2[rows, :] = gobuf[toks].astype(F32).reshape(ROWS, D).astype(BF16)
        return carry

    lax.fori_loop(0, NZ, flatten, 0)

    pl.semaphore_wait(barrier, KA - 1 + 2 * (PB - 1))

    def mean_copy(k):
        peer = (ka + k) % KA
        return pltpu.make_async_remote_copy(
            src_ref=sums.at[peer % 2], dst_ref=means.at[ka], send_sem=mean_s.at[k],
            recv_sem=mean_r.at[ka], device_id={"ka": peer}, device_id_type=MESH,
        )

    def mean_arrival(k):
        peer = (ka + k) % KA
        return pltpu.make_async_remote_copy(
            src_ref=sums.at[c], dst_ref=means.at[peer], send_sem=mean_s.at[k],
            recv_sem=mean_r.at[peer], device_id={"ka": peer}, device_id_type=MESH,
        )

    swap = pltpu.make_async_remote_copy(
        src_ref=deq.at[other], dst_ref=kv_full.at[:, own_rows], send_sem=kvx_s, recv_sem=kvx_r,
        device_id={"ka": sibling}, device_id_type=MESH,
    )
    their_rows = pl.ds(pl.multiple_of(KEYS * other, KEYS), KEYS)
    swapped = pltpu.make_async_remote_copy(
        src_ref=deq.at[other], dst_ref=kv_full.at[:, their_rows], send_sem=kvx_s, recv_sem=kvx_r,
        device_id={"ka": sibling}, device_id_type=MESH,
    )
    for k in FAR_FIRST:
        mean_copy(k).start()
    swap.start()
    swapped.wait_recv()

    lanes = lax.broadcasted_iota(jnp.int32, (CKEYS, D), 1)
    k_ones = jnp.where(lanes < 3 * GROUP, -1.0, 0.0).astype(BF16)
    v_ones = jnp.where((lanes >= 3 * GROUP) & (lanes < 6 * GROUP), -1.0, 0.0).astype(BF16)

    kt[0:D, :] = kv_full[0].astype(F32).T.astype(BF16)
    kt[D:, :] = jnp.ones((16, CKEYS), BF16)
    token = lax.shift_right_logical(lax.broadcasted_iota(jnp.int32, (16, ROWS), 1), 3)
    gap = lax.broadcasted_iota(jnp.int32, (16, ROWS), 0) - token

    def first(i, carry):
        places = []
        for at in range(2):
            s = 2 * i + at
            places.append((at, s, pl.ds(pl.multiple_of(s * ROWS, ROWS), ROWS)))
        for at, s, rows in places:
            extra = mbuf[rows, :]
            k_in = jnp.concatenate([kv_full[0], k_ones], axis=1)
            v_in = jnp.concatenate([kv_full[1], v_ones], axis=1)
            s_all[s] = dot(k_in, jnp.concatenate([q2[rows, :], extra], axis=1), NT)
            dp_all[s] = dot(v_in, jnp.concatenate([go2[rows, :], extra], axis=1), NT)
        for at, s, rows in places:
            limit = TOK * b + SHARE * s - CKEYS * z
            top = jnp.full((16, ROWS), HIDDEN, F32)
            for k0 in range(0, CKEYS, 16):
                a = jnp.where(gap + k0 <= limit, s_all[s, k0:k0 + 16, :] * (inv * LOG2E), HIDDEN)
                s_all[s, k0:k0 + 16, :] = a
                top = jnp.maximum(top, a)
            peak = jnp.max(top, axis=0, keepdims=True)
            stab[s] = peak
            for k0 in range(0, CKEYS, 16):
                w = jnp.exp2(s_all[s, k0:k0 + 16, :] - peak)
                f = w * dp_all[s, k0:k0 + 16, :]
                s_all[s, k0:k0 + 16, :] = w
                dp_all[s, k0:k0 + 16, :] = f
                ds_scr[at, k0:k0 + 16, :] = f.astype(BF16)
        for at, s, rows in places:
            both_sums = dot(kt[...], ds_scr[at], NN)
            dqt[s] = both_sums[0:D]
            totf[s] = both_sums[D:D + 1]
        return carry

    lax.fori_loop(0, NZ // 2, first, 0)

    m_row = lax.broadcasted_iota(jnp.int32, (2 * KEYS, KEYS), 0)
    m_col = lax.broadcasted_iota(jnp.int32, (2 * KEYS, KEYS), 1)
    for h in range(2):
        merge[h] = jnp.where(m_row == 2 * m_col + h, 1.0, 0.0).astype(BF16)

    for k in range(1, KA):
        mean_arrival(k).wait_recv()
    means[ka] = sums[c]
    total = means[0]
    for k in range(1, KA):
        total = total + means[k]
    mean = jnp.broadcast_to(total / (KA * KEYS), (8, D))
    mean_col = jnp.broadcast_to(mean[0:1], (D, D)).T
    m_hi, m_mid, m_lo = split3(mean)
    srow = lax.broadcasted_iota(jnp.int32, (8, D), 0)
    mean_rows = jnp.where(srow == 0, m_hi, jnp.where(srow == 1, m_mid, jnp.where(srow == 2, m_lo, 0.0)))
    mean_rows = jnp.concatenate([mean_rows, jnp.zeros((8, D), F32)], axis=0).astype(BF16)
    acc[...] = jnp.zeros_like(acc)

    def offset(t):
        return jnp.where(t % 2 == 1, (t - 1) // 2 - 3, NZ // 2 - t // 2)

    left = (z + NZ - 1) % NZ
    right = (z + 1) % NZ

    def hop(t, half):
        leftward = half == 0 if t == 0 else t % 2 == 1
        to = left if leftward else right
        if t == 0:
            to = (z + NZ - 2) % NZ if leftward else (z + 2) % NZ
            return pltpu.make_async_remote_copy(
                src_ref=tx.at[t, half], dst_ref=far.at[half], send_sem=tx_s.at[t, half],
                recv_sem=far_r.at[half], device_id={"ka": 2 * to + c}, device_id_type=MESH,
            )
        if t < 5:
            at = t + 2
            return pltpu.make_async_remote_copy(
                src_ref=tx.at[t, half], dst_ref=rx.at[at, half], send_sem=tx_s.at[t, half],
                recv_sem=rx_r.at[at, half], device_id={"ka": 2 * to + c}, device_id_type=MESH,
            )
        side = 0 if leftward else 1
        return pltpu.make_async_remote_copy(
            src_ref=tx.at[t, half], dst_ref=fin.at[side, c], send_sem=tx_s.at[t, half],
            recv_sem=fin_r.at[side, c], device_id={"ka": 2 * to + half}, device_id_type=MESH,
        )

    def arrival(t, half):
        return pltpu.make_async_remote_copy(
            src_ref=tx.at[t, half], dst_ref=rx.at[t, half], send_sem=tx_s.at[t, half],
            recv_sem=rx_r.at[t, half], device_id={"ka": sibling}, device_id_type=MESH,
        )

    def far_arrival(half):
        return pltpu.make_async_remote_copy(
            src_ref=tx.at[0, half], dst_ref=far.at[half], send_sem=tx_s.at[0, half],
            recv_sem=far_r.at[half], device_id={"ka": sibling}, device_id_type=MESH,
        )

    def part(t, half):
        return dqbuf[t, half * HALF:(half + 1) * HALF, :]

    def begin(t, half):
        tx[t, half] = part(t, half).astype(BF16)
        hop(t, half).start()

    def forward(t, half):
        arrival(t, half).wait_recv()
        summed = part(t, half) + rx[t, half].astype(F32)
        if (t, half) in ((3, 0), (4, 1)):
            far_arrival(half).wait_recv()
            summed = summed + far[half].astype(F32)
        tx[t, half] = summed.astype(BF16)
        hop(t, half).start()

    def finish_share(t):
        s = (z + offset(t) + NZ) % NZ
        rows = pl.ds(pl.multiple_of(s * ROWS, ROWS), ROWS)
        shift = jnp.sum(dot(mean_rows, q2[rows, :], NT)[0:8], axis=0, keepdims=True)
        factor = jnp.exp2(stab[s] - shift * (inv * LOG2E))
        gain[s] = factor
        for l0 in range(0, ROWS, D):
            at = slice(l0, l0 + D)
            centred = dqt[s, :, at] - mean_col * totf[s, :, at]
            dqbuf[t, at, :] = (centred * (factor[:, at] * inv)).T

    for t in range(NZ):
        finish_share(t)
        if t == 0:
            begin(0, 0)
            begin(0, 1)
        elif t < 3:
            begin(t, 0)
            begin(t, 1)

    def second(i, carry):
        places = []
        for at in range(2):
            s = 2 * i + at
            places.append((at, s, pl.ds(pl.multiple_of(s * ROWS, ROWS), ROWS)))
        for at, s, rows in places:
            factor = gain[s]
            for k0 in range(0, CKEYS, 16):
                p_scr[at, k0:k0 + 16, :] = (s_all[s, k0:k0 + 16, :] * factor).astype(BF16)
                ds_scr[at, k0:k0 + 16, :] = (dp_all[s, k0:k0 + 16, :] * factor).astype(BF16)
        add_k, add_v = acc[0], acc[1]
        for at, s, rows in places:
            add_k = add_k + dot(ds_scr[at], q2[rows, :], NN)
            add_v = add_v + dot(p_scr[at], go2[rows, :], NN)
        acc[0] = add_k
        acc[1] = add_v
        return carry

    lax.fori_loop(0, NZ // 2, second, 0)

    kvtx[0] = (acc[0] * inv).astype(BF16)
    kvtx[1] = acc[1].astype(BF16)

    def piece_copy(k):
        peer = (b + k) % PB
        return pltpu.make_async_remote_copy(
            src_ref=kvtx.at[:, pl.ds(pl.multiple_of(peer * PIECE, PIECE), PIECE)], dst_ref=kvrx.at[b],
            send_sem=pb_s.at[k], recv_sem=pb_r.at[b], device_id={"pb": peer}, device_id_type=MESH,
        )

    def piece_arrival(k):
        peer = (b + k) % PB
        return pltpu.make_async_remote_copy(
            src_ref=kvtx.at[:, pl.ds(pl.multiple_of(peer * PIECE, PIECE), PIECE)], dst_ref=kvrx.at[peer],
            send_sem=pb_s.at[k], recv_sem=pb_r.at[peer], device_id={"pb": peer}, device_id_type=MESH,
        )

    for k in range(1, PB):
        piece_copy(k).start()

    tx[7, 0] = part(7, 0).astype(BF16)
    tx[7, 1] = part(7, 1).astype(BF16)
    to_sib = pltpu.make_async_remote_copy(
        src_ref=tx.at[7, other], dst_ref=sib, send_sem=tx_s.at[7, 0], recv_sem=sib_r,
        device_id={"ka": sibling}, device_id_type=MESH,
    )
    to_sib.start()

    for which in ((3, 1), (4, 0), (3, 0), (4, 1)):
        forward(*which)

    for k in range(1, PB):
        piece_arrival(k).wait_recv()
    kvrx[b] = kvtx[:, pl.ds(pl.multiple_of(b * PIECE, PIECE), PIECE), :]
    gathered = kvrx[0].astype(F32)
    for k in range(1, PB):
        gathered = gathered + kvrx[k].astype(F32)
    red[...] = gathered.astype(BF16)

    owner = b // (PB // 2)
    slot = b % (PB // 2)
    goal = ag.at[:, c, pl.ds(pl.multiple_of(slot * PIECE, PIECE), PIECE)]

    def spread_copy(k):
        return pltpu.make_async_remote_copy(
            src_ref=red, dst_ref=goal, send_sem=ag_s.at[k], recv_sem=ag_r.at[c, slot],
            device_id={"pb": (b + k) % PB, "ka": 2 * z + owner}, device_id_type=MESH,
        )

    def spread_arrival(h, sl):
        return pltpu.make_async_remote_copy(
            src_ref=red, dst_ref=ag.at[:, h, pl.ds(sl * PIECE, PIECE)], send_sem=ag_s.at[0],
            recv_sem=ag_r.at[h, sl], device_id={"ka": sibling}, device_id_type=MESH,
        )

    for k in range(1, PB):
        spread_copy(k).start()

    @pl.when(owner == c)
    def _():
        ag[:, c, pl.ds(pl.multiple_of(slot * PIECE, PIECE), PIECE), :] = red[...]

    @pl.when(owner != c)
    def _():
        spread_copy(0).start()

    for which in ((5, 1), (6, 0), (5, 0), (6, 1)):
        forward(*which)

    for side in range(2):
        for h in range(2):
            pltpu.make_async_remote_copy(
                src_ref=tx.at[5, 0], dst_ref=fin.at[side, h], send_sem=tx_s.at[5, 0],
                recv_sem=fin_r.at[side, h], device_id={"ka": sibling}, device_id_type=MESH,
            ).wait_recv()
    to_sib.wait_recv()
    mine = dqbuf[7, pl.ds(pl.multiple_of(c * HALF, HALF), HALF), :]
    for h, local in ((c, mine), (other, sib[...].astype(F32))):
        whole = local + fin[0, h].astype(F32) + fin[1, h].astype(F32)
        dq_ref[:, h] = whole.reshape(HALF // GROUP, GROUP, D).astype(BF16)

    for h in range(2):
        for sl in range(PB // 2):
            @pl.when(jnp.logical_not((owner == c) & (slot == sl) & (c == h)))
            def _():
                spread_arrival(h, sl).wait_recv()
    side_by_side = [jnp.concatenate([ag[0, h], ag[1, h]], axis=1) for h in range(2)]
    merged = dot(merge[0], side_by_side[0], NN) + dot(merge[1], side_by_side[1], NN)
    dkv_ref[0] = merged[:, :D].astype(BF16)
    dkv_ref[1] = merged[:, D:].astype(BF16)

    for k in range(1, KA):
        mean_copy(k).wait_send()
    swap.wait_send()
    for t in range(7):
        for half in range(2):
            hop(t, half).wait_send()
    to_sib.wait_send()
    for k in range(1, PB):
        piece_copy(k).wait_send()
        spread_copy(k).wait_send()

    @pl.when(owner != c)
    def _():
        spread_copy(0).wait_send()


def write_out(dq_ref, dkv_ref, dq_hbm, dk_hbm, dv_hbm, sems):
    copies = [
        pltpu.make_async_copy(dq_ref, dq_hbm, sems.at[0]),
        pltpu.make_async_copy(dkv_ref.at[0], dk_hbm, sems.at[1]),
        pltpu.make_async_copy(dkv_ref.at[1], dv_hbm, sems.at[2]),
    ]
    for copy in copies:
        copy.start()
    for copy in copies:
        copy.wait()


def per_device(queries, key_codes, key_scale_powers, values, grad_out, grad_dot, log_totals):
    vmem = pl.BlockSpec(memory_space=pltpu.VMEM)
    anyw = pl.BlockSpec(memory_space=pl.ANY)
    dma = pltpu.SemaphoreType.DMA
    dq, dkv = pl.pallas_call(
        kernel,
        out_shape=(
            pltpu.VMEM((TOK // KA, 2, GROUP, D), BF16),
            pltpu.VMEM((2, 2 * KEYS, D), BF16),
        ),
        in_specs=[anyw] * 7,
        out_specs=(vmem, vmem),
        scratch_shapes=[
            pltpu.VMEM((GROUP, TOK), F32),
            pltpu.VMEM((GROUP, TOK), F32),
            pltpu.VMEM((2 * KEYS, D), BF16),
            pltpu.VMEM((2 * KEYS, D), BF16),
            pltpu.SMEM((2, KEYS // KEYS_PER_SCALE), jnp.int32),
            pltpu.VMEM((2, 2 * KEYS, KEYS), BF16),
            pltpu.VMEM((TOK, GROUP, D), BF16),
            pltpu.VMEM((TOK, GROUP, D), BF16),
            pltpu.VMEM((TOK * GROUP, D), BF16),
            pltpu.VMEM((TOK * GROUP, D), BF16),
            pltpu.VMEM((TOK * GROUP, D), BF16),
            pltpu.VMEM((2, 2, KEYS, D), BF16),
            pltpu.VMEM((2, CKEYS, D), BF16),
            pltpu.VMEM((2, 1, D), F32),
            pltpu.VMEM((KA, 1, D), F32),
            pltpu.VMEM((D + 16, CKEYS), BF16),
            pltpu.VMEM((NZ, CKEYS, ROWS), F32),
            pltpu.VMEM((NZ, CKEYS, ROWS), F32),
            pltpu.VMEM((NZ, 1, ROWS), F32),
            pltpu.VMEM((NZ, 1, ROWS), F32),
            pltpu.VMEM((NZ, 1, ROWS), F32),
            pltpu.VMEM((NZ, D, ROWS), F32),
            pltpu.VMEM((2, CKEYS, ROWS), BF16),
            pltpu.VMEM((2, CKEYS, ROWS), BF16),
            pltpu.VMEM((NZ, ROWS, D), F32),
            pltpu.VMEM((2, CKEYS, D), F32),
            pltpu.VMEM((NZ, 2, HALF, D), BF16),
            pltpu.VMEM((7, 2, HALF, D), BF16),
            pltpu.VMEM((2, HALF, D), BF16),
            pltpu.VMEM((2, 2, HALF, D), BF16),
            pltpu.VMEM((HALF, D), BF16),
            pltpu.VMEM((2, CKEYS, D), BF16),
            pltpu.VMEM((PB, 2, PIECE, D), BF16),
            pltpu.VMEM((2, PIECE, D), BF16),
            pltpu.VMEM((2, 2, KEYS, D), BF16),
            dma((7,)),
            dma,
            dma,
            dma((KA,)),
            dma((KA,)),
            dma((NZ, 2)),
            dma((7, 2)),
            dma((2,)),
            dma((2, 2)),
            dma,
            dma((PB,)),
            dma((PB,)),
            dma((PB,)),
            dma((2, PB // 2)),
        ],
        compiler_params=pltpu.CompilerParams(collective_id=0, has_side_effects=True),
    )(
        queries.reshape(TOK, 2, GROUP, D),
        grad_out.reshape(TOK, 2, GROUP, D),
        log_totals.T,
        grad_dot.T,
        key_codes.reshape(2 * KEYS, D),
        values.reshape(2 * KEYS, D),
        key_scale_powers.T,
    )
    dq, dk, dv = pl.pallas_call(
        write_out,
        out_shape=(
            jax.ShapeDtypeStruct((TOK // KA, 2, GROUP, D), BF16),
            jax.ShapeDtypeStruct((2 * KEYS, D), BF16),
            jax.ShapeDtypeStruct((2 * KEYS, D), BF16),
        ),
        in_specs=[vmem, vmem],
        out_specs=(anyw, anyw, anyw),
        scratch_shapes=[dma((3,))],
        compiler_params=pltpu.CompilerParams(vmem_limit_bytes=4 * 1024 * 1024),
    )(dq, dkv)
    return (
        dq.reshape(TOK // KA, 2 * GROUP, D),
        dk.reshape(KEYS, 2, D),
        dv.reshape(KEYS, 2, D),
    )


def solution(mesh):
    in_specs = (
        P("pb", "ha", None),
        P("ka", "ha", None),
        P("ka", "ha"),
        P("ka", "ha", None),
        P("pb", "ha", None),
        P("pb", "ha"),
        P("pb", "ha"),
    )
    out_specs = (P(("pb", "ka"), "ha", None), P("ka", "ha", None), P("ka", "ha", None))
    return jax.shard_map(
        per_device, mesh=mesh, in_specs=in_specs, out_specs=out_specs, check_vma=False
    )
```

```python
import functools

import jax
import jax.numpy as jnp
from jax import lax
from jax.experimental import pallas as pl
from jax.experimental.pallas import tpu as pltpu
from jax.sharding import PartitionSpec as P

F32 = jnp.float32
BF16 = jnp.bfloat16
MESH = pl.DeviceIdType.MESH
NT = (((1,), (1,)), ((), ()))
NN = (((1,), (0,)), ((), ()))

PB = 8
NZ = 8
KA = 16
TOK = 384
GROUP = 8
D = 128
KEYS = 192
CKEYS = 384
SHARE = 48
ROWS = SHARE * GROUP
HALF = ROWS // 2
PIECE = CKEYS // PB
KEYS_PER_SCALE = 64
LOG2E = 1.4426950408889634
HIDDEN = -1e30
FAR_FIRST = sorted(range(1, KA), key=lambda k: (abs(k - KA // 2), k))


def dot(a, b, dims):
    return lax.dot_general(a, b, dims, preferred_element_type=F32)


def split3(x):
    hi = x.astype(BF16).astype(F32)
    rest = x - hi
    mid = rest.astype(BF16).astype(F32)
    return hi, mid, rest - mid


def kernel(
    q_hbm, go_hbm, tot_hbm, dots_hbm, codes_hbm, vals_hbm, pows_hbm,
    dq_ref, dkv_ref,
    tot_ref, dots_ref, codes_ref, vals_ref, pows_ref, merge,
    qbuf, gobuf, q2, go2, mbuf, deq, kv_full, sums, means, kt, s_all, dp_all,
    stab, totf, gain, dqt, p_scr, ds_scr, dqbuf, acc, tx, rx, far, fin, sib, kvtx, kvrx, red, ag,
    in_sem, kvx_s, kvx_r, mean_s, mean_r, tx_s, rx_r, far_r, fin_r, sib_r,
    pb_s, pb_r, ag_s, ag_r,
):
    b = lax.axis_index("pb")
    ka = lax.axis_index("ka")
    z = ka // 2
    c = ka % 2
    other = 1 - c
    sibling = 2 * z + other
    inv = D ** -0.5

    barrier = pltpu.get_barrier_semaphore()
    for k in FAR_FIRST:
        pl.semaphore_signal(barrier, inc=1, device_id={"ka": (ka + k) % KA}, device_id_type=MESH)
    for k in range(1, PB):
        for core in range(2):
            pl.semaphore_signal(
                barrier, inc=1, device_id={"pb": (b + k) % PB, "ka": 2 * z + core}, device_id_type=MESH
            )

    q_copy = pltpu.make_async_copy(q_hbm.at[:, c], qbuf, in_sem.at[0])
    go_copy = pltpu.make_async_copy(go_hbm.at[:, c], gobuf, in_sem.at[1])
    heads = pl.ds(pl.multiple_of(GROUP * c, GROUP), GROUP)
    loads = [
        pltpu.make_async_copy(codes_hbm, codes_ref, in_sem.at[2]),
        pltpu.make_async_copy(vals_hbm, vals_ref, in_sem.at[3]),
        pltpu.make_async_copy(pows_hbm, pows_ref, in_sem.at[4]),
        pltpu.make_async_copy(tot_hbm.at[heads], tot_ref, in_sem.at[5]),
        pltpu.make_async_copy(dots_hbm.at[heads], dots_ref, in_sem.at[6]),
    ]
    for load in loads:
        load.start()
    q_copy.start()
    go_copy.start()
    for load in loads:
        load.wait()

    both = jnp.concatenate([codes_ref[...], vals_ref[...]], axis=1)
    for h in range(2):
        row = lax.broadcasted_iota(jnp.int32, (KEYS, 2 * KEYS), 0)
        col = lax.broadcasted_iota(jnp.int32, (KEYS, 2 * KEYS), 1)
        pick = jnp.where(col == 2 * row + h, 1.0, 0.0).astype(BF16)
        picked = dot(pick, both, NN)
        total = jnp.zeros((1, D), F32)
        for blk in range(KEYS // KEYS_PER_SCALE):
            at = slice(blk * KEYS_PER_SCALE, (blk + 1) * KEYS_PER_SCALE)
            power = jnp.full((KEYS_PER_SCALE, D), pows_ref[h, blk], jnp.int32).astype(F32)
            scaled = picked[at, :D] * jnp.exp2(power)
            total = total + jnp.sum(scaled, axis=0, keepdims=True)
            deq[h, 0, at, :] = scaled.astype(BF16)
        deq[h, 1, :, :] = picked[:, D:].astype(BF16)
        sums[h] = total

    own_rows = pl.ds(pl.multiple_of(KEYS * c, KEYS), KEYS)
    kv_full[:, own_rows, :] = deq[c]

    pieces = split3(tot_ref[...] * (D ** 0.5)) + split3(dots_ref[...])
    stacked = jnp.concatenate(list(pieces) + [jnp.zeros((D - 6 * GROUP, TOK), F32)], axis=0)
    by_token = stacked.T
    lane = lax.broadcasted_iota(jnp.int32, (GROUP, D), 1)
    sub = lax.broadcasted_iota(jnp.int32, (GROUP, D), 0)
    own_lane = jnp.where((lane & (GROUP - 1)) == sub, 1.0, 0.0)
    for s in range(NZ):
        at = by_token[s * SHARE:(s + 1) * SHARE]
        spread = at[:, None, :] * own_lane[None]
        mbuf[s * ROWS:(s + 1) * ROWS, :] = spread.reshape(ROWS, D).astype(BF16)

    q_copy.wait()
    go_copy.wait()

    def flatten(s, carry):
        toks = pl.ds(s * SHARE, SHARE)
        rows = pl.ds(pl.multiple_of(s * ROWS, ROWS), ROWS)
        q2[rows, :] = qbuf[toks].astype(F32).reshape(ROWS, D).astype(BF16)
        go2[rows, :] = gobuf[toks].astype(F32).reshape(ROWS, D).astype(BF16)
        return carry

    lax.fori_loop(0, NZ, flatten, 0)

    pl.semaphore_wait(barrier, KA - 1 + 2 * (PB - 1))

    def mean_copy(k):
        peer = (ka + k) % KA
        return pltpu.make_async_remote_copy(
            src_ref=sums.at[peer % 2], dst_ref=means.at[ka], send_sem=mean_s.at[k],
            recv_sem=mean_r.at[ka], device_id={"ka": peer}, device_id_type=MESH,
        )

    def mean_arrival(k):
        peer = (ka + k) % KA
        return pltpu.make_async_remote_copy(
            src_ref=sums.at[c], dst_ref=means.at[peer], send_sem=mean_s.at[k],
            recv_sem=mean_r.at[peer], device_id={"ka": peer}, device_id_type=MESH,
        )

    swap = pltpu.make_async_remote_copy(
        src_ref=deq.at[other], dst_ref=kv_full.at[:, own_rows], send_sem=kvx_s, recv_sem=kvx_r,
        device_id={"ka": sibling}, device_id_type=MESH,
    )
    their_rows = pl.ds(pl.multiple_of(KEYS * other, KEYS), KEYS)
    swapped = pltpu.make_async_remote_copy(
        src_ref=deq.at[other], dst_ref=kv_full.at[:, their_rows], send_sem=kvx_s, recv_sem=kvx_r,
        device_id={"ka": sibling}, device_id_type=MESH,
    )
    for k in FAR_FIRST:
        mean_copy(k).start()
    swap.start()
    swapped.wait_recv()

    lanes = lax.broadcasted_iota(jnp.int32, (CKEYS, D), 1)
    k_ones = jnp.where(lanes < 3 * GROUP, -1.0, 0.0).astype(BF16)
    v_ones = jnp.where((lanes >= 3 * GROUP) & (lanes < 6 * GROUP), -1.0, 0.0).astype(BF16)

    kt[0:D, :] = kv_full[0].astype(F32).T.astype(BF16)
    kt[D:, :] = jnp.ones((16, CKEYS), BF16)
    token = lax.shift_right_logical(lax.broadcasted_iota(jnp.int32, (16, ROWS), 1), 3)
    gap = lax.broadcasted_iota(jnp.int32, (16, ROWS), 0) - token

    def first(i, carry):
        places = []
        for at in range(2):
            s = 2 * i + at
            places.append((at, s, pl.ds(pl.multiple_of(s * ROWS, ROWS), ROWS)))
        for at, s, rows in places:
            extra = mbuf[rows, :]
            k_in = jnp.concatenate([kv_full[0], k_ones], axis=1)
            v_in = jnp.concatenate([kv_full[1], v_ones], axis=1)
            s_all[s] = dot(k_in, jnp.concatenate([q2[rows, :], extra], axis=1), NT)
            dp_all[s] = dot(v_in, jnp.concatenate([go2[rows, :], extra], axis=1), NT)
        for at, s, rows in places:
            limit = TOK * b + SHARE * s - CKEYS * z
            top = jnp.full((16, ROWS), HIDDEN, F32)
            for k0 in range(0, CKEYS, 16):
                a = jnp.where(gap + k0 <= limit, s_all[s, k0:k0 + 16, :] * (inv * LOG2E), HIDDEN)
                s_all[s, k0:k0 + 16, :] = a
                top = jnp.maximum(top, a)
            peak = jnp.max(top, axis=0, keepdims=True)
            stab[s] = peak
            for k0 in range(0, CKEYS, 16):
                w = jnp.exp2(s_all[s, k0:k0 + 16, :] - peak)
                f = w * dp_all[s, k0:k0 + 16, :]
                s_all[s, k0:k0 + 16, :] = w
                dp_all[s, k0:k0 + 16, :] = f
                ds_scr[at, k0:k0 + 16, :] = f.astype(BF16)
        for at, s, rows in places:
            both_sums = dot(kt[...], ds_scr[at], NN)
            dqt[s] = both_sums[0:D]
            totf[s] = both_sums[D:D + 1]
        return carry

    lax.fori_loop(0, NZ // 2, first, 0)

    m_row = lax.broadcasted_iota(jnp.int32, (2 * KEYS, KEYS), 0)
    m_col = lax.broadcasted_iota(jnp.int32, (2 * KEYS, KEYS), 1)
    for h in range(2):
        merge[h] = jnp.where(m_row == 2 * m_col + h, 1.0, 0.0).astype(BF16)

    for k in range(1, KA):
        mean_arrival(k).wait_recv()
    means[ka] = sums[c]
    total = means[0]
    for k in range(1, KA):
        total = total + means[k]
    mean = jnp.broadcast_to(total / (KA * KEYS), (8, D))
    mean_col = jnp.broadcast_to(mean[0:1], (D, D)).T
    m_hi, m_mid, m_lo = split3(mean)
    srow = lax.broadcasted_iota(jnp.int32, (8, D), 0)
    mean_rows = jnp.where(srow == 0, m_hi, jnp.where(srow == 1, m_mid, jnp.where(srow == 2, m_lo, 0.0)))
    mean_rows = jnp.concatenate([mean_rows, jnp.zeros((8, D), F32)], axis=0).astype(BF16)
    acc[...] = jnp.zeros_like(acc)

    def offset(t):
        return jnp.where(t % 2 == 1, (t - 1) // 2 - 3, NZ // 2 - t // 2)

    left = (z + NZ - 1) % NZ
    right = (z + 1) % NZ

    def hop(t, half):
        leftward = half == 0 if t == 0 else t % 2 == 1
        to = left if leftward else right
        if t == 0:
            to = (z + NZ - 2) % NZ if leftward else (z + 2) % NZ
            return pltpu.make_async_remote_copy(
                src_ref=tx.at[t, half], dst_ref=far.at[half], send_sem=tx_s.at[t, half],
                recv_sem=far_r.at[half], device_id={"ka": 2 * to + c}, device_id_type=MESH,
            )
        if t < 5:
            at = t + 2
            return pltpu.make_async_remote_copy(
                src_ref=tx.at[t, half], dst_ref=rx.at[at, half], send_sem=tx_s.at[t, half],
                recv_sem=rx_r.at[at, half], device_id={"ka": 2 * to + c}, device_id_type=MESH,
            )
        side = 0 if leftward else 1
        return pltpu.make_async_remote_copy(
            src_ref=tx.at[t, half], dst_ref=fin.at[side, c], send_sem=tx_s.at[t, half],
            recv_sem=fin_r.at[side, c], device_id={"ka": 2 * to + half}, device_id_type=MESH,
        )

    def arrival(t, half):
        return pltpu.make_async_remote_copy(
            src_ref=tx.at[t, half], dst_ref=rx.at[t, half], send_sem=tx_s.at[t, half],
            recv_sem=rx_r.at[t, half], device_id={"ka": sibling}, device_id_type=MESH,
        )

    def far_arrival(half):
        return pltpu.make_async_remote_copy(
            src_ref=tx.at[0, half], dst_ref=far.at[half], send_sem=tx_s.at[0, half],
            recv_sem=far_r.at[half], device_id={"ka": sibling}, device_id_type=MESH,
        )

    def part(t, half):
        return dqbuf[t, half * HALF:(half + 1) * HALF, :]

    def begin(t, half):
        tx[t, half] = part(t, half).astype(BF16)
        hop(t, half).start()

    def forward(t, half):
        arrival(t, half).wait_recv()
        summed = part(t, half) + rx[t, half].astype(F32)
        if (t, half) in ((3, 0), (4, 1)):
            far_arrival(half).wait_recv()
            summed = summed + far[half].astype(F32)
        tx[t, half] = summed.astype(BF16)
        hop(t, half).start()

    def find_gain(t):
        s = (z + offset(t) + NZ) % NZ
        rows = pl.ds(pl.multiple_of(s * ROWS, ROWS), ROWS)
        shift = jnp.sum(dot(mean_rows, q2[rows, :], NT)[0:8], axis=0, keepdims=True)
        gain[s] = jnp.exp2(stab[s] - shift * (inv * LOG2E))

    def finish_share(t):
        s = (z + offset(t) + NZ) % NZ
        factor = gain[s]
        for l0 in range(0, ROWS, D):
            at = slice(l0, l0 + D)
            centred = dqt[s, :, at] - mean_col * totf[s, :, at]
            dqbuf[t, at, :] = (centred * (factor[:, at] * inv)).T

    for t in range(3):
        find_gain(t)
        finish_share(t)
        begin(t, 0)
        begin(t, 1)
    for t in range(3, NZ):
        find_gain(t)

    def second(i, carry):
        places = []
        for at in range(2):
            s = 2 * i + at
            places.append((at, s, pl.ds(pl.multiple_of(s * ROWS, ROWS), ROWS)))
        for at, s, rows in places:
            factor = gain[s]
            for k0 in range(0, CKEYS, 16):
                p_scr[at, k0:k0 + 16, :] = (s_all[s, k0:k0 + 16, :] * factor).astype(BF16)
                ds_scr[at, k0:k0 + 16, :] = (dp_all[s, k0:k0 + 16, :] * factor).astype(BF16)
        add_k, add_v = acc[0], acc[1]
        for at, s, rows in places:
            add_k = add_k + dot(ds_scr[at], q2[rows, :], NN)
            add_v = add_v + dot(p_scr[at], go2[rows, :], NN)
        acc[0] = add_k
        acc[1] = add_v
        return carry

    lax.fori_loop(0, NZ // 2, second, 0)

    kvtx[0] = (acc[0] * inv).astype(BF16)
    kvtx[1] = acc[1].astype(BF16)

    def piece_copy(k):
        peer = (b + k) % PB
        return pltpu.make_async_remote_copy(
            src_ref=kvtx.at[:, pl.ds(pl.multiple_of(peer * PIECE, PIECE), PIECE)], dst_ref=kvrx.at[b],
            send_sem=pb_s.at[k], recv_sem=pb_r.at[b], device_id={"pb": peer}, device_id_type=MESH,
        )

    def piece_arrival(k):
        peer = (b + k) % PB
        return pltpu.make_async_remote_copy(
            src_ref=kvtx.at[:, pl.ds(pl.multiple_of(peer * PIECE, PIECE), PIECE)], dst_ref=kvrx.at[peer],
            send_sem=pb_s.at[k], recv_sem=pb_r.at[peer], device_id={"pb": peer}, device_id_type=MESH,
        )

    for k in range(1, PB):
        piece_copy(k).start()

    for t in range(3, NZ):
        finish_share(t)

    tx[7, 0] = part(7, 0).astype(BF16)
    tx[7, 1] = part(7, 1).astype(BF16)
    to_sib = pltpu.make_async_remote_copy(
        src_ref=tx.at[7, other], dst_ref=sib, send_sem=tx_s.at[7, 0], recv_sem=sib_r,
        device_id={"ka": sibling}, device_id_type=MESH,
    )
    to_sib.start()

    for which in ((3, 1), (4, 0), (3, 0), (4, 1)):
        forward(*which)

    for k in range(1, PB):
        piece_arrival(k).wait_recv()
    kvrx[b] = kvtx[:, pl.ds(pl.multiple_of(b * PIECE, PIECE), PIECE), :]
    gathered = kvrx[0].astype(F32)
    for k in range(1, PB):
        gathered = gathered + kvrx[k].astype(F32)
    red[...] = gathered.astype(BF16)

    owner = b // (PB // 2)
    slot = b % (PB // 2)
    goal = ag.at[:, c, pl.ds(pl.multiple_of(slot * PIECE, PIECE), PIECE)]

    def spread_copy(k):
        return pltpu.make_async_remote_copy(
            src_ref=red, dst_ref=goal, send_sem=ag_s.at[k], recv_sem=ag_r.at[c, slot],
            device_id={"pb": (b + k) % PB, "ka": 2 * z + owner}, device_id_type=MESH,
        )

    def spread_arrival(h, sl):
        return pltpu.make_async_remote_copy(
            src_ref=red, dst_ref=ag.at[:, h, pl.ds(sl * PIECE, PIECE)], send_sem=ag_s.at[0],
            recv_sem=ag_r.at[h, sl], device_id={"ka": sibling}, device_id_type=MESH,
        )

    for k in range(1, PB):
        spread_copy(k).start()

    @pl.when(owner == c)
    def _():
        ag[:, c, pl.ds(pl.multiple_of(slot * PIECE, PIECE), PIECE), :] = red[...]

    @pl.when(owner != c)
    def _():
        spread_copy(0).start()

    for which in ((5, 1), (6, 0), (5, 0), (6, 1)):
        forward(*which)

    for side in range(2):
        for h in range(2):
            pltpu.make_async_remote_copy(
                src_ref=tx.at[5, 0], dst_ref=fin.at[side, h], send_sem=tx_s.at[5, 0],
                recv_sem=fin_r.at[side, h], device_id={"ka": sibling}, device_id_type=MESH,
            ).wait_recv()
    to_sib.wait_recv()
    mine = dqbuf[7, pl.ds(pl.multiple_of(c * HALF, HALF), HALF), :]
    for h, local in ((c, mine), (other, sib[...].astype(F32))):
        whole = local + fin[0, h].astype(F32) + fin[1, h].astype(F32)
        dq_ref[:, h] = whole.reshape(HALF // GROUP, GROUP, D).astype(BF16)

    for h in range(2):
        for sl in range(PB // 2):
            @pl.when(jnp.logical_not((owner == c) & (slot == sl) & (c == h)))
            def _():
                spread_arrival(h, sl).wait_recv()
    side_by_side = [jnp.concatenate([ag[0, h], ag[1, h]], axis=1) for h in range(2)]
    merged = dot(merge[0], side_by_side[0], NN) + dot(merge[1], side_by_side[1], NN)
    dkv_ref[0] = merged[:, :D].astype(BF16)
    dkv_ref[1] = merged[:, D:].astype(BF16)

    for k in range(1, KA):
        mean_copy(k).wait_send()
    swap.wait_send()
    for t in range(7):
        for half in range(2):
            hop(t, half).wait_send()
    to_sib.wait_send()
    for k in range(1, PB):
        piece_copy(k).wait_send()
        spread_copy(k).wait_send()

    @pl.when(owner != c)
    def _():
        spread_copy(0).wait_send()


def write_out(dq_ref, dkv_ref, dq_hbm, dk_hbm, dv_hbm, sems):
    copies = [
        pltpu.make_async_copy(dq_ref, dq_hbm, sems.at[0]),
        pltpu.make_async_copy(dkv_ref.at[0], dk_hbm, sems.at[1]),
        pltpu.make_async_copy(dkv_ref.at[1], dv_hbm, sems.at[2]),
    ]
    for copy in copies:
        copy.start()
    for copy in copies:
        copy.wait()


def per_device(queries, key_codes, key_scale_powers, values, grad_out, grad_dot, log_totals):
    vmem = pl.BlockSpec(memory_space=pltpu.VMEM)
    anyw = pl.BlockSpec(memory_space=pl.ANY)
    dma = pltpu.SemaphoreType.DMA
    dq, dkv = pl.pallas_call(
        kernel,
        out_shape=(
            pltpu.VMEM((TOK // KA, 2, GROUP, D), BF16),
            pltpu.VMEM((2, 2 * KEYS, D), BF16),
        ),
        in_specs=[anyw] * 7,
        out_specs=(vmem, vmem),
        scratch_shapes=[
            pltpu.VMEM((GROUP, TOK), F32),
            pltpu.VMEM((GROUP, TOK), F32),
            pltpu.VMEM((2 * KEYS, D), BF16),
            pltpu.VMEM((2 * KEYS, D), BF16),
            pltpu.SMEM((2, KEYS // KEYS_PER_SCALE), jnp.int32),
            pltpu.VMEM((2, 2 * KEYS, KEYS), BF16),
            pltpu.VMEM((TOK, GROUP, D), BF16),
            pltpu.VMEM((TOK, GROUP, D), BF16),
            pltpu.VMEM((TOK * GROUP, D), BF16),
            pltpu.VMEM((TOK * GROUP, D), BF16),
            pltpu.VMEM((TOK * GROUP, D), BF16),
            pltpu.VMEM((2, 2, KEYS, D), BF16),
            pltpu.VMEM((2, CKEYS, D), BF16),
            pltpu.VMEM((2, 1, D), F32),
            pltpu.VMEM((KA, 1, D), F32),
            pltpu.VMEM((D + 16, CKEYS), BF16),
            pltpu.VMEM((NZ, CKEYS, ROWS), F32),
            pltpu.VMEM((NZ, CKEYS, ROWS), F32),
            pltpu.VMEM((NZ, 1, ROWS), F32),
            pltpu.VMEM((NZ, 1, ROWS), F32),
            pltpu.VMEM((NZ, 1, ROWS), F32),
            pltpu.VMEM((NZ, D, ROWS), F32),
            pltpu.VMEM((2, CKEYS, ROWS), BF16),
            pltpu.VMEM((2, CKEYS, ROWS), BF16),
            pltpu.VMEM((NZ, ROWS, D), F32),
            pltpu.VMEM((2, CKEYS, D), F32),
            pltpu.VMEM((NZ, 2, HALF, D), BF16),
            pltpu.VMEM((7, 2, HALF, D), BF16),
            pltpu.VMEM((2, HALF, D), BF16),
            pltpu.VMEM((2, 2, HALF, D), BF16),
            pltpu.VMEM((HALF, D), BF16),
            pltpu.VMEM((2, CKEYS, D), BF16),
            pltpu.VMEM((PB, 2, PIECE, D), BF16),
            pltpu.VMEM((2, PIECE, D), BF16),
            pltpu.VMEM((2, 2, KEYS, D), BF16),
            dma((7,)),
            dma,
            dma,
            dma((KA,)),
            dma((KA,)),
            dma((NZ, 2)),
            dma((7, 2)),
            dma((2,)),
            dma((2, 2)),
            dma,
            dma((PB,)),
            dma((PB,)),
            dma((PB,)),
            dma((2, PB // 2)),
        ],
        compiler_params=pltpu.CompilerParams(collective_id=0, has_side_effects=True),
    )(
        queries.reshape(TOK, 2, GROUP, D),
        grad_out.reshape(TOK, 2, GROUP, D),
        log_totals.T,
        grad_dot.T,
        key_codes.reshape(2 * KEYS, D),
        values.reshape(2 * KEYS, D),
        key_scale_powers.T,
    )
    dq, dk, dv = pl.pallas_call(
        write_out,
        out_shape=(
            jax.ShapeDtypeStruct((TOK // KA, 2, GROUP, D), BF16),
            jax.ShapeDtypeStruct((2 * KEYS, D), BF16),
            jax.ShapeDtypeStruct((2 * KEYS, D), BF16),
        ),
        in_specs=[vmem, vmem],
        out_specs=(anyw, anyw, anyw),
        scratch_shapes=[dma((3,))],
        compiler_params=pltpu.CompilerParams(vmem_limit_bytes=4 * 1024 * 1024),
    )(dq, dkv)
    return (
        dq.reshape(TOK // KA, 2 * GROUP, D),
        dk.reshape(KEYS, 2, D),
        dv.reshape(KEYS, 2, D),
    )


def solution(mesh):
    in_specs = (
        P("pb", "ha", None),
        P("ka", "ha", None),
        P("ka", "ha"),
        P("ka", "ha", None),
        P("pb", "ha", None),
        P("pb", "ha"),
        P("pb", "ha"),
    )
    out_specs = (P(("pb", "ka"), "ha", None), P("ka", "ha", None), P("ka", "ha", None))
    return jax.shard_map(
        per_device, mesh=mesh, in_specs=in_specs, out_specs=out_specs, check_vma=False
    )
```
